16 devices in a mesh: right: 4 (over z, y), left: 4 (over x, core).
Axes of the slice: x: 2, y: 2, z: 2, core: 2. Of those that a mesh axis runs over, the one named last changes fastest.
Arguments:
- psi_init: float32 [2048, 2, 2, 512], P('left', None, None, 'right')
- left_env: float32 [2048, 20, 2048], P('left')
- right_env: float32 [512, 20, 512], P('right')
- mpo_two: float32 [20, 20, 2, 2, 2, 2], replicated
Outputs:
- output 1: float32 [4], replicated
- output 2: float32 [4], replicated
- output 3: float32 [2048, 2, 2, 512], P('left', None, None, 'right')
All inputs are finite; a program needn't handle non-finite values.
Results may differ from the reference program's by a relative error of at most 0.001.
Values sent between devices are 32-bit elements.
A program may use at most 1 GiB of HBM per device.

```python
import jax
import jax.numpy as jnp
from jax import lax

PHYS_DIM = 2
MPO_DIM = 20
LEFT_BOND = 2048
RIGHT_BOND = 512
LANCZOS_STEPS = 4
ROW_BLOCK = min(LEFT_BOND, 512)
ROW_COUNT = LEFT_BOND // ROW_BLOCK
PREC_HIGH = lax.Precision.HIGHEST


def sym_env(key_main, key_diag, bond_size):
    rand_part = jax.random.normal(key_main, (bond_size, MPO_DIM, bond_size), jnp.float32)
    shifts = jax.random.uniform(key_diag, (MPO_DIM,), jnp.float32, 0.5, 1.5)
    eye_mat = jnp.eye(bond_size, dtype=jnp.float32)
    sym_part = (rand_part + jnp.transpose(rand_part, (2, 1, 0))) * (2.0 * bond_size) ** -0.5
    return sym_part + shifts[None, :, None] * eye_mat[:, None, :]


def draw_mpo(key_main, key_diag):
    shape_six = (MPO_DIM, MPO_DIM, PHYS_DIM, PHYS_DIM, PHYS_DIM, PHYS_DIM)
    rand_part = jax.random.normal(key_main, shape_six, jnp.float32)
    sym_part = (rand_part + jnp.transpose(rand_part, (0, 1, 4, 5, 2, 3))) * (2.0 * MPO_DIM * MPO_DIM * PHYS_DIM * PHYS_DIM) ** -0.5
    weights = jax.random.uniform(key_diag, (MPO_DIM, MPO_DIM), jnp.float32, 0.5, 1.5) / (MPO_DIM * MPO_DIM)
    eye_phys = jnp.eye(PHYS_DIM * PHYS_DIM, dtype=jnp.float32).reshape(PHYS_DIM, PHYS_DIM, PHYS_DIM, PHYS_DIM)
    return sym_part + weights[:, :, None, None, None, None] * eye_phys[None, None]


def setup_inputs(seed: int = 0) -> dict:
    key_list = jax.random.split(jax.random.key(seed), 7)
    psi_init = jax.random.normal(key_list[0], (LEFT_BOND, PHYS_DIM, PHYS_DIM, RIGHT_BOND), jnp.float32)
    left_env = sym_env(key_list[1], key_list[2], LEFT_BOND)
    right_env = sym_env(key_list[3], key_list[4], RIGHT_BOND)
    mpo_two = draw_mpo(key_list[5], key_list[6])
    return {'psi_init': psi_init, 'left_env': left_env, 'right_env': right_env, 'mpo_two': mpo_two}


def apply_ham(vec_in, left_env, right_env, mpo_two):
    def one_block(block_idx):
        env_block = lax.dynamic_slice_in_dim(left_env, block_idx * ROW_BLOCK, ROW_BLOCK, axis=2)
        t_one = jnp.einsum('alc,astb->lcstb', env_block, vec_in, precision=PREC_HIGH)
        t_two = jnp.einsum('lcstb,lrstuv->cbruv', t_one, mpo_two, precision=PREC_HIGH)
        return jnp.einsum('cbruv,brd->cuvd', t_two, right_env, precision=PREC_HIGH)
    out_blocks = lax.map(one_block, jnp.arange(ROW_COUNT))
    return out_blocks.reshape(LEFT_BOND, PHYS_DIM, PHYS_DIM, RIGHT_BOND)


def reference(psi_init, left_env, right_env, mpo_two):
    elem_count = LEFT_BOND * PHYS_DIM * PHYS_DIM * RIGHT_BOND
    start_vec = psi_init * jnp.sqrt(elem_count / jnp.sum(psi_init * psi_init))

    def lanczos_step(step_carry, unused):
        vec_prev, vec_cur, beta_prev = step_carry
        next_vec = apply_ham(vec_cur, left_env, right_env, mpo_two)
        alpha_val = jnp.sum(vec_cur * next_vec) / elem_count
        next_vec = next_vec - alpha_val * vec_cur - beta_prev * vec_prev
        beta_val = jnp.sqrt(jnp.sum(next_vec * next_vec) / elem_count)
        return (vec_cur, next_vec / beta_val, beta_val), (alpha_val, beta_val)

    start_carry = (jnp.zeros_like(start_vec), start_vec, jnp.zeros((), jnp.float32))
    end_carry, step_outs = lax.scan(lanczos_step, start_carry, None, length=LANCZOS_STEPS)
    return step_outs[0], step_outs[1], end_carry[1]
```

```python
import jax
import jax.numpy as jnp
from jax import lax
from jax.sharding import PartitionSpec as P

LANCZOS_STEPS = 4
PREC_HIGH = lax.Precision.HIGHEST


def solution(mesh):
    device_count = mesh.shape['left'] * mesh.shape['right']

    def global_dot(vec_one, vec_two):
        return lax.psum(jnp.sum(vec_one * vec_two), ('left', 'right'))

    def apply_ham(vec_block, left_env, right_cols, mpo_two):
        gathered = lax.all_gather(vec_block, 'right', axis=3, tiled=True)
        u_one = jnp.einsum('astb,brd->rstad', gathered, right_cols, precision=PREC_HIGH, preferred_element_type=jnp.float32)
        u_two = jnp.einsum('rstad,lrstuv->aluvd', u_one, mpo_two, precision=PREC_HIGH, preferred_element_type=jnp.float32)
        partial_out = jnp.einsum('alc,aluvd->cuvd', left_env, u_two, precision=PREC_HIGH, preferred_element_type=jnp.float32)
        return lax.psum_scatter(partial_out, 'left', scatter_dimension=0, tiled=True)

    def lanczos(psi_block, left_env, right_env, mpo_two):
        right_cols = lax.all_to_all(right_env, 'right', split_axis=2, concat_axis=0, tiled=True)
        elem_count = psi_block.size * device_count
        vec_cur = psi_block * jnp.sqrt(elem_count / global_dot(psi_block, psi_block))
        vec_prev = vec_cur
        beta_prev = jnp.float32(0.0)
        alpha_list = []
        beta_list = []
        for step_idx in range(LANCZOS_STEPS):
            next_vec = apply_ham(vec_cur, left_env, right_cols, mpo_two)
            alpha_val = global_dot(vec_cur, next_vec) / elem_count
            next_vec = next_vec - alpha_val * vec_cur
            if step_idx > 0:
                next_vec = next_vec - beta_prev * vec_prev
            beta_val = jnp.sqrt(global_dot(next_vec, next_vec) / elem_count)
            vec_prev = vec_cur
            vec_cur = next_vec / beta_val
            beta_prev = beta_val
            alpha_list.append(alpha_val)
            beta_list.append(beta_val)
        return jnp.stack(alpha_list), jnp.stack(beta_list), vec_cur

    return jax.shard_map(
        lanczos,
        mesh=mesh,
        in_specs=(P('left', None, None, 'right'), P('left', None, None), P('right', None, None), P()),
        out_specs=(P(), P(), P('left', None, None, 'right')),
        check_vma=False,
    )
```

```python
import functools

import jax
import jax.numpy as jnp
from jax import lax
from jax.experimental import pallas as pl
from jax.experimental.pallas import tpu as pltpu
from jax.sharding import PartitionSpec as P

STEPS = 4
W = 20
S = 4
BF = jnp.bfloat16
F32 = jnp.float32
VM_LIMIT = 67043328


class Cfg:
    def __init__(self, lt=256, bl=128, row_chunk=128):
        self.lt = lt
        self.a = 2 * lt
        self.bl = bl
        self.nb = 4 * bl
        self.kb = self.nb // 2
        self.groups = bl // 16
        self.rows = 4 * bl
        self.rc = row_chunk
        self.nl = max(lt // 128, 1)
        self.elems = float(4 * self.a * S * self.nb)


def split3(x):
    one = x.astype(BF)
    rest = x - one.astype(F32)
    two = rest.astype(BF)
    return one, two, (rest - two.astype(F32)).astype(BF)


def remote(src, dst, send_sem, recv_sem, right, left):
    return pltpu.make_async_remote_copy(
        src_ref=src, dst_ref=dst, send_sem=send_sem, recv_sem=recv_sem,
        device_id={'right': right, 'left': left}, device_id_type=pl.DeviceIdType.MESH)


def enter(me):
    barrier = pltpu.get_barrier_semaphore()

    @pl.loop(1, 16)
    def _(off):
        peer = lax.rem(me + off, 16)
        pl.semaphore_signal(barrier, 1, device_id={'right': peer // 4, 'left': lax.rem(peer, 4)},
                            device_id_type=pl.DeviceIdType.MESH)

    pl.semaphore_wait(barrier, 15)


def all_sum(part, k, me, out_ref, in_ref, send_sem, recv_sem):
    out_ref[k] = part
    in_ref[k, me] = part

    def copy(peer, slot):
        return remote(out_ref.at[k], in_ref.at[k, slot], send_sem.at[k, peer], recv_sem.at[k, slot],
                      peer // 4, lax.rem(peer, 4))

    @pl.loop(1, 16)
    def _(off):
        copy(lax.rem(me + off, 16), me).start()

    @pl.loop(1, 16)
    def _(off):
        peer = lax.rem(me + off, 16)
        copy(peer, peer).wait_recv()

    total = in_ref[k, 0]
    for i in range(1, 16):
        total = total + in_ref[k, i]

    @pl.loop(1, 16)
    def _(off):
        copy(lax.rem(me + off, 16), me).wait_send()

    return jnp.sum(jnp.sum(total, axis=1, keepdims=True), axis=0, keepdims=True)


def fold(x):
    r, c = x.shape
    if c % 128 == 0:
        x = jnp.sum(x.reshape(r // 8, 8, c), axis=0)
        acc = x[:, :128]
        for i in range(1, c // 128):
            acc = acc + x[:, i * 128:(i + 1) * 128]
        return acc
    return jnp.full((8, 128), jnp.sum(x) / 1024.0, F32)


def prep_kernel(cfg, l3, rb3, psi, ls, rtf, qg0, nrm,
                ibuf, obuf, rbv, rst, ars, arr,
                isem, osem, lsem, ar_s, ar_r, ps_s, ps_r, rh_s, rh_r, ro_s, ro_r, rf_s, rf_r):
    me_r = lax.axis_index('right')
    me_l = lax.axis_index('left')
    me = me_r * 4 + me_l
    core = lax.rem(me_l, 2)
    mate = me_l + 1 - 2 * core
    bl, lt, rc = cfg.bl, cfg.lt, cfg.rc
    half = W // 2
    nchunk = cfg.a // rc
    total = W * nchunk

    load_r = pltpu.make_async_copy(rb3, rbv, lsem.at[0])
    load_r.start()

    def get(n, slot):
        return pltpu.make_async_copy(l3.at[n // nchunk, pl.ds(pl.multiple_of(lax.rem(n, nchunk) * rc, rc), rc), :],
                                     ibuf.at[slot], isem.at[slot])

    def put(n, slot):
        return pltpu.make_async_copy(
            obuf.at[slot],
            ls.at[:, :, n // nchunk, :, pl.ds(pl.multiple_of(lax.rem(n, nchunk) * rc, rc), rc), :], osem.at[slot])

    get(0, 0).start()
    get(1, 1).start()
    enter(me)

    def psi_copy(off):
        peer = lax.rem(me_r + off, 4)
        return remote(psi, qg0.at[:, :, pl.ds(pl.multiple_of(me_r * bl, bl), bl), :], ps_s.at[off], ps_r.at[me_r], peer, me_l)

    def psi_from(off):
        peer = lax.rem(me_r + off, 4)
        return remote(psi, qg0.at[:, :, pl.ds(pl.multiple_of(peer * bl, bl), bl), :], ps_s.at[off], ps_r.at[peer], peer, me_l)

    def r_half(off):
        peer = lax.rem(me_r + off, 4)
        return remote(rst.at[peer, pl.ds(core * half, half)],
                      rtf.at[pl.ds(core * half, half), :, pl.ds(pl.multiple_of(me_r * bl, bl), bl)],
                      rh_s.at[off], rh_r.at[me_r], peer, me_l)

    def r_from(off):
        peer = lax.rem(me_r + off, 4)
        return remote(rst.at[peer, pl.ds(core * half, half)],
                      rtf.at[pl.ds(core * half, half), :, pl.ds(pl.multiple_of(peer * bl, bl), bl)],
                      rh_s.at[off], rh_r.at[peer], peer, me_l)

    def r_fwd(off, mine):
        peer = lax.rem(me_r + off, 4)
        where = core if mine else 1 - core
        part = rtf.at[pl.ds(where * half, half), :, pl.ds(pl.multiple_of(peer * bl, bl), bl)]
        return remote(part, part, rf_s.at[off], rf_r.at[off], me_r, mate)

    def r_own():
        return remote(rst.at[me_r], rtf.at[:, :, pl.ds(pl.multiple_of(me_r * bl, bl), bl)], ro_s.at[0], ro_r.at[0], me_r, mate)

    own_psi = pltpu.make_async_copy(psi, qg0.at[:, :, pl.ds(pl.multiple_of(me_r * bl, bl), bl), :], lsem.at[1])
    own_psi.start()

    load_r.wait()
    for j in range(4):
        @pl.loop(0, W)
        def _(r):
            rst[j, r] = rbv[r, :, j * bl:(j + 1) * bl].T
    for off in range(1, 4):
        r_half(off).start()
    r_own().start()
    for off in range(1, 4):
        psi_copy(off).start()

    part = jnp.zeros((8, 128), F32)
    for h in range(2):
        for s in range(S):
            x = psi[h, s]
            part = part + fold(x * x)
    tot = all_sum(part, 0, me, ars, arr, ar_s, ar_r)
    nrm[...] = jnp.broadcast_to(tot, (8, 128))

    forward_at = (total // 4) * 3

    @pl.loop(0, total)
    def _(n):
        slot = lax.rem(n, 2)

        @pl.when(n == forward_at)
        def _():
            for off in range(1, 4):
                r_from(off).wait_recv()
            for off in range(1, 4):
                r_fwd(off, True).start()

        get(n, slot).wait()

        @pl.when(n >= 2)
        def _():
            put(n - 2, slot).wait()

        for d in range(4):
            for h in range(2):
                c0 = (2 * d + h) * lt
                for k, v in enumerate(split3(ibuf[slot, :, c0:c0 + lt])):
                    obuf[slot, d, h, k] = v

        put(n, slot).start()

        @pl.when(n + 2 < total)
        def _():
            get(n + 2, slot).start()

    put(total - 2, total % 2).wait()
    put(total - 1, (total - 1) % 2).wait()
    own_psi.wait()
    for off in range(1, 4):
        psi_from(off).wait_recv()
        psi_copy(off).wait_send()
        r_half(off).wait_send()
        r_fwd(off, False).wait_recv()
        r_fwd(off, True).wait_send()
    r_own().wait_recv()
    r_own().wait_send()


def prep(cfg, l3, rb3, psi):
    a, bl, nb, lt = cfg.a, cfg.bl, cfg.nb, cfg.lt
    hbm = pl.BlockSpec(memory_space=pl.ANY)
    vm = pl.BlockSpec(memory_space=pltpu.VMEM)
    dma = pltpu.SemaphoreType.DMA
    return pl.pallas_call(
        functools.partial(prep_kernel, cfg),
        out_shape=(
            jax.ShapeDtypeStruct((4, 2, W, 3, a, lt), BF),
            jax.ShapeDtypeStruct((W, bl, nb), F32),
            jax.ShapeDtypeStruct((2, S, nb, lt), F32),
            jax.ShapeDtypeStruct((8, 128), F32),
        ),
        in_specs=[hbm, hbm, vm],
        out_specs=(hbm, hbm, hbm, vm),
        scratch_shapes=[
            pltpu.VMEM((2, cfg.rc, 4 * a), F32),
            pltpu.VMEM((2, 4, 2, 3, cfg.rc, lt), BF),
            pltpu.VMEM((W, bl, nb), F32),
            pltpu.VMEM((4, W, bl, bl), F32),
            pltpu.VMEM((1, 8, 128), F32),
            pltpu.VMEM((1, 16, 8, 128), F32),
            dma((2,)), dma((2,)), dma((2,)), dma((1, 16)), dma((1, 16)),
            dma((4,)), dma((4,)), dma((4,)), dma((4,)), dma((1,)), dma((1,)), dma((4,)), dma((4,)),
        ],
        compiler_params=pltpu.CompilerParams(collective_id=0, has_side_effects=True, vmem_limit_bytes=VM_LIMIT),
    )(l3, rb3, psi)


NL = 4


def steps_kernel(cfg, ls, rtf, qg0, wl, nrm, out_v, out_s,
                 u2, rts, vg, qg, lb, sb, rb0, yb, xs, ub0, ub1, ob, vp, acc, rcb, cf, al, ars, arr,
                 lsem, rcsem, qsem, ar_s, ar_r, rs_s, rs_r, ag_s, ag_r, credit):
    lt, bl, nb, kb, rows, groups = cfg.lt, cfg.bl, cfg.nb, cfg.kb, cfg.rows, cfg.groups
    nl, lw = cfg.nl, cfg.lt // cfg.nl
    me_r = lax.axis_index('right')
    me_l = lax.axis_index('left')
    me = me_r * 4 + me_l
    core = lax.rem(me_l, 2)
    chip = me_l // 2
    mate = chip * 2 + 1 - core
    across = (1 - chip) * 2 + core
    own = pl.ds(pl.multiple_of(me_r * bl, bl), bl)
    trips = W // NL
    low = lax.broadcasted_iota(jnp.int32, (8, lt), 0) < 4

    load_q = pltpu.make_async_copy(qg0, qg, qsem)
    load_q.start()

    def get_r(i, slot):
        return pltpu.make_async_copy(rtf.at[:, pl.ds(pl.multiple_of(i * 8, 8), 8), :], rcb.at[slot], rcsem.at[slot])

    get_r(0, 0).start()
    enter(me)
    vg[...] = jnp.zeros(vg.shape, F32)
    ub1[...] = jnp.zeros(ub1.shape, F32)
    lowb = lax.broadcasted_iota(jnp.int32, (8, nb), 0) < 4

    @pl.loop(0, bl // 8)
    def _(i):
        slot = lax.rem(i, 2)

        @pl.when(i + 1 < bl // 8)
        def _():
            get_r(i + 1, 1 - slot).start()

        get_r(i, slot).wait()
        one = jnp.transpose(rcb[slot, 0:8], (1, 0, 2))
        two = jnp.transpose(rcb[slot, 8:16], (1, 0, 2))
        tail = rcb[slot, 16:20]
        tail = jnp.transpose(jnp.concatenate([tail, tail], axis=0), (1, 0, 2))
        for quad in range(2):
            b0 = 4 * quad
            parts = []
            for b in range(b0, b0 + 4):
                parts += [one[b], two[b]]
            parts += [jnp.where(lowb, tail[b0], tail[b0 + 1]), jnp.where(lowb, tail[b0 + 2], tail[b0 + 3])]
            for k, v in enumerate(split3(jnp.concatenate(parts, axis=0))):
                rts[k, pl.ds(pl.multiple_of(i * 160 + 80 * quad, 16), 80), :] = v

    norm = jnp.sqrt(nrm[...] / cfg.elems)
    cf[0] = jnp.zeros((8, 128), F32)
    cf[1] = 1.0 / norm
    cf[2] = norm
    load_q.wait()

    def place(n):
        h = n // (4 * trips)
        who = lax.rem(n // trips, 4)
        to = lax.rem(chip + 1 - who // 2, 2) * 2 + lax.rem(core + 1 - lax.rem(who, 2), 2)
        return to, h, lax.rem(n, trips)

    def get_l(n):
        d, h, p = place(n)
        slot = lax.rem(n + 1, 2)
        return pltpu.make_async_copy(ls.at[d, h, pl.ds(p * NL, NL)], lb.at[slot, :, :, :cfg.a], lsem.at[slot])

    def ag_copy(h, off):
        peer = lax.rem(me_r + off, 4)
        return remote(qg.at[h, :, own, :], qg.at[h, :, own, :], ag_s.at[h, off], ag_r.at[h, me_r], peer, me_l)

    def ag_from(h, off):
        peer = lax.rem(me_r + off, 4)
        there = qg.at[h, :, pl.ds(pl.multiple_of(peer * bl, bl), bl), :]
        return remote(there, there, ag_s.at[h, off], ag_r.at[h, peer], peer, me_l)

    def coef(i, shape):
        one = cf[i, 0:1, 0:1]
        return jnp.broadcast_to(one, shape)

    def update(h, j):
        @pl.when(j > 0)
        def _():
            for off in range(1, 4):
                ag_from(h, off).wait_recv()
                ag_copy(h, off).wait_send()

        for s in range(S):
            vp[h, s] = vg[h, s, own, :]
        chunk = min(64, nb)

        @pl.loop(0, S * (nb // chunk))
        def _(i):
            s = i // (nb // chunk)
            at = pl.ds(pl.multiple_of(lax.rem(i, nb // chunk) * chunk, chunk), chunk)
            new = (qg[h, s, at, :] - coef(0, (chunk, lt)) * vg[h, s, at, :]) * coef(1, (chunk, lt))
            vg[h, s, at, :] = new
            for k, v in enumerate(split3(new)):
                lb[0, s, k, at, :] = v

        @pl.when(j < STEPS - 1)
        def _():
            for off in range(1, 4):
                pl.semaphore_signal(credit.at[h], 1, device_id={'right': lax.rem(me_r + off, 4), 'left': me_l},
                                    device_id_type=pl.DeviceIdType.MESH)

    def w_tile(ub, quad, i):
        base = 80 * quad
        pair = base + 64 + 8 * (i // 2)
        parts = [ub[s, base + 16 * i:base + 16 * i + 16, :] for s in range(S)]
        for s in (0, 2):
            one, two = ub[s, pair:pair + 8, :], ub[s + 1, pair:pair + 8, :]
            if i % 2 == 0:
                parts.append(jnp.where(low, one, pltpu.roll(two, 4, 0)))
            else:
                parts.append(jnp.where(low, pltpu.roll(one, 4, 0), two))
        x = jnp.concatenate(parts, axis=0)
        return jnp.concatenate([*split3(x), jnp.zeros((16, lt), BF)], axis=0)

    def w_finish(quad, g, h):
        even, odd = [], []
        for i in range(W // 2):
            v = [ob[b, 8 * i:8 * i + 8, :] for b in range(4)]
            for dst, b0 in ((even, 0), (even, 2)):
                dst.append(jnp.where(low, v[b0], pltpu.roll(v[b0 + 1], 4, 0)))
            for dst, b0 in ((odd, 0), (odd, 2)):
                dst.append(jnp.where(low, pltpu.roll(v[b0], 4, 0), v[b0 + 1]))
        at = pl.ds(pl.multiple_of(g * 64 + 16 * quad, 16), 16)
        col = pl.ds(pl.multiple_of(h * lt, lt), lt)
        for first, lst in ((0, even), (1, odd)):
            for k, v in enumerate(split3(jnp.concatenate(lst, axis=0))):
                for i in range(W // 2):
                    u2[2 * i + first, k, at, col] = v[16 * i:16 * i + 16]

    def group(it, ub_new, ub_old, do_r=True):
        before = lax.rem(it + 2 * groups - 1, 2 * groups)
        gw, hw = lax.rem(before, groups), before // groups
        at = pl.ds(pl.multiple_of(lax.rem(it, groups) * (16 * W), 16 * W), 16 * W)
        for s in range(S):
            if do_r:
                total = None
                for k in range(3):
                    for i in range(3 - k):
                        term = jnp.dot(rts[i, at, :], lb[0, s, k, :nb, :], preferred_element_type=F32)
                        total = term if total is None else total + term
                ub_new[s] = total
            for i in range(4):
                y = jnp.dot(wl[...], w_tile(ub_old, s, i), preferred_element_type=F32)
                ob[i] = (y[:4 * W] + y[4 * W:8 * W]) + y[8 * W:]
            w_finish(s, gw, hw)

    def l_trip(n, p):
        get_l(n).wait()

        @pl.when(n + 1 < 8 * trips)
        def _():
            get_l(n + 1).start()

        slot = lax.rem(n + 1, 2)
        total = None
        for m in range(NL):
            for k in range(3):
                for i in range(3 - k):
                    term = jnp.dot(u2[p * NL + m, i], lb[slot, m, k, :cfg.a, :], preferred_element_type=F32)
                    total = term if total is None else total + term
        acc[...] += total

    def rs_copy(k, h):
        dst = (rb0, xs.at[h], yb)[k]
        i = 1 + h if k == 1 else (0 if k == 0 else 3)
        return remote(sb.at[k], dst, rs_s.at[k], rs_r.at[i], me_r, across if k == 1 else mate)

    def l_phase(h, j):
        for who in range(4):
            acc[...] = jnp.zeros((rows, lt), F32)

            @pl.loop(0, trips)
            def _(p):
                l_trip((h * 4 + who) * trips + p, p)

            if who == 1:
                rs_copy(0, h).wait_recv()
            if who == 2:
                rs_copy(0, h).wait_send()
            if who == 3:
                rs_copy(2, h).wait_recv()
                rs_copy(1, h).wait_recv()
            for i in range(nl):
                y = acc[:, i * lw:(i + 1) * lw]
                if who == 1:
                    y = y + rb0[i]
                if who < 3:
                    sb[who, i] = y
                else:
                    yb[i] = (y + yb[i]) + xs[h, i]
            if who < 3:
                rs_copy(who, h).start()

        rs_copy(1, h).wait_send()
        rs_copy(2, h).wait_send()
        beta = coef(2, (bl, lt))
        for t in range(S):
            w = jnp.concatenate([yb[i, pl.ds(t, bl, stride=4), :] for i in range(nl)], axis=1)
            al[...] += fold(w * vg[h, t, own, :])
            qg[h, t, own, :] = w - beta * vp[h, t]

        @pl.when(j < STEPS - 1)
        def _():
            pl.semaphore_wait(credit.at[h], 3)
            for off in range(1, 4):
                ag_copy(h, off).start()

    @pl.loop(0, STEPS)
    def _(j):
        get_l(0).start()

        @pl.loop(0, groups)
        def _(p):
            @pl.when(lax.rem(p, groups // 2) == 0)
            def _():
                update(p // (groups // 2), j)

            group(2 * p, ub0, ub1)
            group(2 * p + 1, ub1, ub0)

        group(2 * groups, ub0, ub1, do_r=False)
        al[...] = jnp.zeros((8, 128), F32)

        @pl.loop(0, 2)
        def _(h):
            l_phase(h, j)

        alpha = jnp.broadcast_to(all_sum(al[...], 0, me, ars, arr, ar_s, ar_r), (8, 128)) / cfg.elems
        cf[0] = alpha
        out_s[j] = alpha
        part = jnp.zeros((8, 128), F32)
        for h in range(2):
            for s in range(S):
                w = qg[h, s, own, :] - coef(0, (bl, lt)) * vg[h, s, own, :]
                part = part + fold(w * w)
        beta = jnp.sqrt(jnp.broadcast_to(all_sum(part, 1, me, ars, arr, ar_s, ar_r), (8, 128)) / cfg.elems)
        cf[1] = 1.0 / beta
        cf[2] = beta
        out_s[STEPS + j] = beta

    for h in range(2):
        for s in range(S):
            out_v[h, s] = (qg[h, s, own, :] - coef(0, (bl, lt)) * vg[h, s, own, :]) * coef(1, (bl, lt))


def steps(cfg, ls, rtf, qg0, wl, nrm):
    lt, bl, nb, rows = cfg.lt, cfg.bl, cfg.nb, cfg.rows
    hbm = pl.BlockSpec(memory_space=pl.ANY)
    vm = pl.BlockSpec(memory_space=pltpu.VMEM)
    dma = pltpu.SemaphoreType.DMA
    block = (cfg.nl, rows, lt // cfg.nl)
    scratch = [
        pltpu.VMEM((W, 3, rows, cfg.a), BF),
        pltpu.VMEM((3, W * bl, nb), BF),
        pltpu.VMEM((2, S, nb, lt), F32),
        pltpu.VMEM((2, S, nb, lt), F32),
        pltpu.VMEM((2, NL, 3, max(cfg.a, nb), lt), BF),
        pltpu.VMEM((3, *block), F32),
        pltpu.VMEM(block, F32),
        pltpu.VMEM(block, F32),
        pltpu.VMEM((2, *block), F32),
        pltpu.VMEM((S, 16 * W, lt), F32),
        pltpu.VMEM((S, 16 * W, lt), F32),
        pltpu.VMEM((4, 4 * W, lt), F32),
        pltpu.VMEM((2, S, bl, lt), F32),
        pltpu.VMEM((rows, lt), F32),
        pltpu.VMEM((2, W, 8, nb), F32),
        pltpu.VMEM((3, 8, 128), F32),
        pltpu.VMEM((8, 128), F32),
        pltpu.VMEM((2, 8, 128), F32),
        pltpu.VMEM((2, 16, 8, 128), F32),
        dma((2,)), dma((2,)), dma, dma((2, 16)), dma((2, 16)), dma((3,)), dma((4,)), dma((2, 4)), dma((2, 4)),
        pltpu.SemaphoreType.REGULAR((2,)),
    ]
    return pl.pallas_call(
        functools.partial(steps_kernel, cfg),
        out_shape=(
            jax.ShapeDtypeStruct((2, S, bl, lt), F32),
            jax.ShapeDtypeStruct((2 * STEPS, 8, 128), F32),
        ),
        in_specs=[hbm, hbm, hbm, vm, vm],
        out_specs=(vm, vm),
        scratch_shapes=scratch,
        compiler_params=pltpu.CompilerParams(collective_id=1, has_side_effects=True, vmem_limit_bytes=VM_LIMIT),
    )(ls, rtf, qg0, wl, nrm)


def mpo_rows(mpo_two):
    w = mpo_two.reshape(W, W, S, S).transpose(0, 3, 2, 1)
    w = jnp.concatenate([w[..., :16].reshape(W * S, 64), w[..., 16:].reshape(W * S, 16)], axis=1)
    one = lax.reduce_precision(w, 8, 7)
    two = lax.reduce_precision(w - one, 8, 7)
    three = w - one - two
    none = jnp.zeros_like(w)
    left = jnp.concatenate([
        jnp.concatenate([one, one, one], 1),
        jnp.concatenate([two, two, none], 1),
        jnp.concatenate([three, none, none], 1)], 0)
    return jnp.pad(left, ((0, 0), (0, 16))).astype(BF)


def build(mesh, cfg):
    def lanczos(psi_block, left_env, right_env, mpo_two):
        lt, a, bl = cfg.lt, cfg.a, cfg.bl
        l3 = jnp.transpose(left_env, (1, 0, 2))
        rb3 = jnp.transpose(right_env, (1, 0, 2))
        psi = psi_block.reshape(2, lt, S, bl).transpose(0, 2, 3, 1)
        wl = mpo_rows(mpo_two)
        ls, rtf, qg0, nrm = prep(cfg, l3, rb3, psi)
        vec, scal = steps(cfg, ls, rtf, qg0, wl, nrm)
        vec = vec.transpose(0, 3, 1, 2).reshape(psi_block.shape)
        return scal[:STEPS, 0, 0], scal[STEPS:, 0, 0], vec

    return jax.shard_map(
        lanczos,
        mesh=mesh,
        in_specs=(P('left', None, None, 'right'), P('left', None, None), P('right', None, None), P()),
        out_specs=(P(), P(), P('left', None, None, 'right')),
        check_vma=False,
    )


def solution(mesh):
    return build(mesh, Cfg())
```

```python
import functools

import jax
import jax.numpy as jnp
from jax import lax
from jax.experimental import pallas as pl
from jax.experimental.pallas import tpu as pltpu
from jax.sharding import PartitionSpec as P

STEPS = 4
W = 20
S = 4
BF = jnp.bfloat16
F32 = jnp.float32
VM_LIMIT = 67043328


class Cfg:
    def __init__(self, lt=256, bl=128):
        self.lt = lt
        self.a = 2 * lt
        self.bl = bl
        self.nb = 4 * bl
        self.kb = self.nb // 2
        self.groups = bl // 16
        self.rows = 4 * bl
        self.nl = max(lt // 128, 1)
        self.elems = float(4 * self.a * S * self.nb)


def split3(x):
    one = x.astype(BF)
    rest = x - one.astype(F32)
    two = rest.astype(BF)
    return one, two, (rest - two.astype(F32)).astype(BF)


def remote(src, dst, send_sem, recv_sem, right, left):
    return pltpu.make_async_remote_copy(
        src_ref=src, dst_ref=dst, send_sem=send_sem, recv_sem=recv_sem,
        device_id={'right': right, 'left': left}, device_id_type=pl.DeviceIdType.MESH)


def enter(me):
    barrier = pltpu.get_barrier_semaphore()

    @pl.loop(1, 16)
    def _(off):
        peer = lax.rem(me + off, 16)
        pl.semaphore_signal(barrier, 1, device_id={'right': peer // 4, 'left': lax.rem(peer, 4)},
                            device_id_type=pl.DeviceIdType.MESH)

    pl.semaphore_wait(barrier, 15)


def all_sum(part, k, me, out_ref, in_ref, send_sem, recv_sem):
    out_ref[k] = part
    in_ref[k, me] = part

    def copy(peer, slot):
        return remote(out_ref.at[k], in_ref.at[k, slot], send_sem.at[k, peer], recv_sem.at[k, slot],
                      peer // 4, lax.rem(peer, 4))

    @pl.loop(1, 16)
    def _(off):
        copy(lax.rem(me + off, 16), me).start()

    @pl.loop(1, 16)
    def _(off):
        peer = lax.rem(me + off, 16)
        copy(peer, peer).wait_recv()

    total = in_ref[k, 0]
    for i in range(1, 16):
        total = total + in_ref[k, i]

    @pl.loop(1, 16)
    def _(off):
        copy(lax.rem(me + off, 16), me).wait_send()

    return jnp.sum(jnp.sum(total, axis=1, keepdims=True), axis=0, keepdims=True)


def fold(x):
    r, c = x.shape
    if c % 128 == 0:
        x = jnp.sum(x.reshape(r // 8, 8, c), axis=0)
        acc = x[:, :128]
        for i in range(1, c // 128):
            acc = acc + x[:, i * 128:(i + 1) * 128]
        return acc
    return jnp.full((8, 128), jnp.sum(x) / 1024.0, F32)


CH = 5


def kernel(cfg, l3, rbt, psi, wl, out_v, out_s, rtf,
           u2, rts, vgs, vg, qg, lb, sb, rb0, yb, xs, ub0, ub1, ob, vp, acc, rcb, cf, al, ars, arr,
           lsem, rcsem, qsem, ar_s, ar_r, rs_s, rs_r, ag_s, ag_r, rh_s, rh_r, ro_s, ro_r, rf_s, rf_r, credit):
    lt, bl, nb, kb, rows, groups = cfg.lt, cfg.bl, cfg.nb, cfg.kb, cfg.rows, cfg.groups
    nl, lw = cfg.nl, cfg.lt // cfg.nl
    me_r = lax.axis_index('right')
    me_l = lax.axis_index('left')
    me = me_r * 4 + me_l
    core = lax.rem(me_l, 2)
    chip = me_l // 2
    mate = chip * 2 + 1 - core
    across = (1 - chip) * 2 + core
    own = pl.ds(pl.multiple_of(me_r * bl, bl), bl)
    half = W // 2
    trips = W // CH
    low = lax.broadcasted_iota(jnp.int32, (8, lt), 0) < 4

    def get_l(n):
        tile = lax.rem(n // trips, 8)
        h, who = tile // 4, lax.rem(tile, 4)
        to = lax.rem(chip + 1 - who // 2, 2) * 2 + lax.rem(core + 1 - lax.rem(who, 2), 2)
        col = pl.ds(pl.multiple_of((2 * to + h) * lt, lt), lt)
        slot = lax.rem(n, 2)
        return pltpu.make_async_copy(l3.at[pl.ds(lax.rem(n, trips) * CH, CH), :, col], lb.at[slot], lsem.at[slot])

    def ag_copy(h, off):
        peer = lax.rem(me_r + off, 4)
        return remote(qg.at[h, :, own, :], qg.at[h, :, own, :], ag_s.at[h, off], ag_r.at[h, me_r], peer, me_l)

    def ag_from(h, off):
        peer = lax.rem(me_r + off, 4)
        there = qg.at[h, :, pl.ds(pl.multiple_of(peer * bl, bl), bl), :]
        return remote(there, there, ag_s.at[h, off], ag_r.at[h, peer], peer, me_l)

    def coef(i, shape):
        one = cf[i, 0:1, 0:1]
        return jnp.broadcast_to(one, shape)

    def update(h, j):
        for off in range(1, 4):
            ag_from(h, off).wait_recv()
            ag_copy(h, off).wait_send()

        for s in range(S):
            vp[h, s] = vg[h, s, own, :]
        chunk = min(256, nb)

        @pl.loop(0, S * (nb // chunk))
        def _(i):
            s = i // (nb // chunk)
            at = pl.ds(pl.multiple_of(lax.rem(i, nb // chunk) * chunk, chunk), chunk)
            new = (qg[h, s, at, :] - coef(0, (chunk, lt)) * vg[h, s, at, :]) * coef(1, (chunk, lt))
            vg[h, s, at, :] = new
            for k, v in enumerate(split3(new)):
                vgs[k, s, at, :] = v

        @pl.when(j < STEPS - 1)
        def _():
            for off in range(1, 4):
                pl.semaphore_signal(credit.at[h], 1, device_id={'right': lax.rem(me_r + off, 4), 'left': me_l},
                                    device_id_type=pl.DeviceIdType.MESH)

    def w_tile(ub, quad, i):
        base = 80 * quad
        pair = base + 64 + 8 * (i // 2)
        parts = [ub[s, base + 16 * i:base + 16 * i + 16, :] for s in range(S)]
        for s in (0, 2):
            one, two = ub[s, pair:pair + 8, :], ub[s + 1, pair:pair + 8, :]
            if i % 2 == 0:
                parts.append(jnp.where(low, one, pltpu.roll(two, 4, 0)))
            else:
                parts.append(jnp.where(low, pltpu.roll(one, 4, 0), two))
        x = jnp.concatenate(parts, axis=0)
        return jnp.concatenate([*split3(x), jnp.zeros((16, lt), BF)], axis=0)

    def w_finish(quad, g, h):
        even, odd = [], []
        for i in range(W // 2):
            v = [ob[b, 8 * i:8 * i + 8, :] for b in range(4)]
            for dst, b0 in ((even, 0), (even, 2)):
                dst.append(jnp.where(low, v[b0], pltpu.roll(v[b0 + 1], 4, 0)))
            for dst, b0 in ((odd, 0), (odd, 2)):
                dst.append(jnp.where(low, pltpu.roll(v[b0], 4, 0), v[b0 + 1]))
        at = pl.ds(pl.multiple_of(g * 64 + 16 * quad, 16), 16)
        col = pl.ds(pl.multiple_of(h * lt, lt), lt)
        for first, lst in ((0, even), (1, odd)):
            for k, v in enumerate(split3(jnp.concatenate(lst, axis=0))):
                for i in range(W // 2):
                    u2[2 * i + first, k, at, col] = v[16 * i:16 * i + 16]

    def group(it, ub_new, ub_old, do_r=True):
        before = lax.rem(it + 2 * groups - 1, 2 * groups)
        gw, hw = lax.rem(before, groups), before // groups
        at = pl.ds(pl.multiple_of(lax.rem(it, groups) * (16 * W), 16 * W), 16 * W)
        for s in range(S):
            if do_r:
                total = None
                for k in range(3):
                    for i in range(3 - k):
                        term = jnp.dot(rts[i, at, :], vgs[k, s], preferred_element_type=F32)
                        total = term if total is None else total + term
                ub_new[s] = total
            for i in range(4):
                y = jnp.dot(wl[...], w_tile(ub_old, s, i), preferred_element_type=F32)
                ob[i] = (y[:4 * W] + y[4 * W:8 * W]) + y[8 * W:]
            w_finish(s, gw, hw)

    def l_trip(n):
        get_l(n).wait()
        get_l(n + 1).start()
        slot, l0 = lax.rem(n, 2), lax.rem(n, trips) * CH
        total = None
        for m in range(CH):
            right = split3(lb[slot, m])
            for k in range(3):
                for i in range(3 - k):
                    term = jnp.dot(u2[l0 + m, i], right[k], preferred_element_type=F32)
                    total = term if total is None else total + term
        acc[...] += total

    def rs_copy(k, h):
        dst = (rb0, xs.at[h], yb)[k]
        i = 1 + h if k == 1 else (0 if k == 0 else 3)
        return remote(sb.at[k], dst, rs_s.at[k], rs_r.at[i], me_r, across if k == 1 else mate)

    def part_of(i):
        return acc[:, i * lw:(i + 1) * lw]

    def send_on(n, j):
        h, who = n // 4, lax.rem(n, 4)

        @pl.when(who == 0)
        def _():
            for i in range(nl):
                sb[0, i] = part_of(i)
            rs_copy(0, h).start()

        @pl.when(who == 1)
        def _():
            rs_copy(0, h).wait_recv()
            for i in range(nl):
                sb[1, i] = part_of(i) + rb0[i]
            rs_copy(1, h).start()

        @pl.when(who == 2)
        def _():
            rs_copy(0, h).wait_send()
            for i in range(nl):
                sb[2, i] = part_of(i)
            rs_copy(2, h).start()

        @pl.when(who == 3)
        def _():
            finish(h, j)

    def finish(h, j):
        rs_copy(2, h).wait_recv()
        rs_copy(1, h).wait_recv()
        for i in range(nl):
            yb[i] = (part_of(i) + yb[i]) + xs[h, i]
        rs_copy(1, h).wait_send()
        rs_copy(2, h).wait_send()
        beta = coef(2, (bl, lt))
        for t in range(S):
            w = jnp.concatenate([yb[i, pl.ds(t, bl, stride=4), :] for i in range(nl)], axis=1)
            al[...] += fold(w * vg[h, t, own, :])
            qg[h, t, own, :] = w - beta * vp[h, t]

        @pl.when(j < STEPS - 1)
        def _():
            pl.semaphore_wait(credit.at[h], 3)
            for off in range(1, 4):
                ag_copy(h, off).start()

    own_psi = pltpu.make_async_copy(psi, qg.at[:, :, own, :], qsem)
    own_psi.start()

    def get_r(i, slot):
        return pltpu.make_async_copy(rtf.at[:, pl.ds(pl.multiple_of(i * 8, 8), 8), :], rcb.at[slot], rcsem.at[slot])

    def r_half(off, peer):
        to = lax.rem(me_r + off, 4)
        part = pl.ds(core * half, half)
        return remote(rbt.at[part, pl.ds(pl.multiple_of(to * bl, bl), bl), :],
                      rtf.at[part, :, pl.ds(pl.multiple_of(peer * bl, bl), bl)], rh_s.at[off], rh_r.at[peer], to, me_l)

    def r_pass(off, which):
        peer = lax.rem(me_r + off, 4)
        part = rtf.at[pl.ds(which * half, half), :, pl.ds(pl.multiple_of(peer * bl, bl), bl)]
        return remote(part, part, rf_s.at[off], rf_r.at[off], me_r, mate)

    def r_own():
        return remote(rbt.at[:, own, :], rtf.at[:, :, own], ro_s.at[0], ro_r.at[0], me_r, mate)

    enter(me)
    for off in range(1, 4):
        r_half(off, me_r).start()
    r_own().start()
    own_psi.wait()
    for h in range(2):
        for off in range(1, 4):
            ag_copy(h, off).start()
    get_l(0).start()

    part = jnp.zeros((8, 128), F32)
    for h in range(2):
        for s in range(S):
            x = qg[h, s, own, :]
            part = part + fold(x * x)
    norm = jnp.sqrt(jnp.broadcast_to(all_sum(part, 0, me, ars, arr, ar_s, ar_r), (8, 128)) / cfg.elems)
    cf[0] = jnp.zeros((8, 128), F32)
    cf[1] = 1.0 / norm
    cf[2] = norm
    vg[...] = jnp.zeros(vg.shape, F32)
    ub1[...] = jnp.zeros(ub1.shape, F32)
    lowb = lax.broadcasted_iota(jnp.int32, (8, nb), 0) < 4

    for off in range(1, 4):
        r_half(off, lax.rem(me_r + off, 4)).wait_recv()
        r_pass(off, core).start()
    r_own().wait_recv()
    for off in range(1, 4):
        r_pass(off, 1 - core).wait_recv()

    @pl.loop(0, bl // 8)
    def _(i):
        slot = 0
        get_r(i, slot).start()
        get_r(i, slot).wait()
        one = jnp.transpose(rcb[slot, 0:8], (1, 0, 2))
        two = jnp.transpose(rcb[slot, 8:16], (1, 0, 2))
        tail = rcb[slot, 16:20]
        tail = jnp.transpose(jnp.concatenate([tail, tail], axis=0), (1, 0, 2))
        for quad in range(2):
            b0 = 4 * quad
            parts = []
            for b in range(b0, b0 + 4):
                parts += [one[b], two[b]]
            parts += [jnp.where(lowb, tail[b0], tail[b0 + 1]), jnp.where(lowb, tail[b0 + 2], tail[b0 + 3])]
            for k, v in enumerate(split3(jnp.concatenate(parts, axis=0))):
                rts[k, pl.ds(pl.multiple_of(i * 160 + 80 * quad, 16), 80), :] = v

    for off in range(1, 4):
        r_half(off, me_r).wait_send()
        r_pass(off, core).wait_send()
    r_own().wait_send()

    @pl.loop(0, STEPS)
    def _(j):
        @pl.loop(0, groups)
        def _(p):
            @pl.when(lax.rem(p, groups // 2) == 0)
            def _():
                update(p // (groups // 2), j)

            group(2 * p, ub0, ub1)
            group(2 * p + 1, ub1, ub0)

        group(2 * groups, ub0, ub1, do_r=False)
        al[...] = jnp.zeros((8, 128), F32)

        acc[...] = jnp.zeros((rows, lt), F32)

        @pl.loop(0, 8 * trips)
        def _(n):
            l_trip(n)

            @pl.when(lax.rem(n, trips) == trips - 1)
            def _():
                send_on(n // trips, j)
                acc[...] = jnp.zeros((rows, lt), F32)

        alpha = jnp.broadcast_to(all_sum(al[...], 0, me, ars, arr, ar_s, ar_r), (8, 128)) / cfg.elems
        cf[0] = alpha
        out_s[j] = alpha
        part = jnp.zeros((8, 128), F32)
        for h in range(2):
            for s in range(S):
                w = qg[h, s, own, :] - coef(0, (bl, lt)) * vg[h, s, own, :]
                part = part + fold(w * w)
        beta = jnp.sqrt(jnp.broadcast_to(all_sum(part, 1, me, ars, arr, ar_s, ar_r), (8, 128)) / cfg.elems)
        cf[1] = 1.0 / beta
        cf[2] = beta
        out_s[STEPS + j] = beta

    get_l(0).wait()
    for h in range(2):
        for s in range(S):
            qg[h, s, own, :] = (qg[h, s, own, :] - coef(0, (bl, lt)) * vg[h, s, own, :]) * coef(1, (bl, lt))
    result = pltpu.make_async_copy(qg.at[:, :, own, :], out_v, qsem)
    result.start()
    result.wait()


def steps(cfg, l3, rbt, psi, wl):
    lt, bl, nb, rows = cfg.lt, cfg.bl, cfg.nb, cfg.rows
    hbm = pl.BlockSpec(memory_space=pl.ANY)
    vm = pl.BlockSpec(memory_space=pltpu.VMEM)
    dma = pltpu.SemaphoreType.DMA
    block = (cfg.nl, rows, lt // cfg.nl)
    scratch = [
        pltpu.VMEM((W, 3, rows, cfg.a), BF),
        pltpu.VMEM((3, W * bl, nb), BF),
        pltpu.VMEM((3, S, nb, lt), BF),
        pltpu.VMEM((2, S, nb, lt), F32),
        pltpu.VMEM((2, S, nb, lt), F32),
        pltpu.VMEM((2, CH, cfg.a, lt), F32),
        pltpu.VMEM((3, *block), F32),
        pltpu.VMEM(block, F32),
        pltpu.VMEM(block, F32),
        pltpu.VMEM((2, *block), F32),
        pltpu.VMEM((S, 16 * W, lt), F32),
        pltpu.VMEM((S, 16 * W, lt), F32),
        pltpu.VMEM((4, 4 * W, lt), F32),
        pltpu.VMEM((2, S, bl, lt), F32),
        pltpu.VMEM((rows, lt), F32),
        pltpu.VMEM((1, W, 8, nb), F32),
        pltpu.VMEM((3, 8, 128), F32),
        pltpu.VMEM((8, 128), F32),
        pltpu.VMEM((2, 8, 128), F32),
        pltpu.VMEM((2, 16, 8, 128), F32),
        dma((2,)), dma((2,)), dma, dma((2, 16)), dma((2, 16)), dma((3,)), dma((4,)), dma((2, 4)), dma((2, 4)),
        dma((4,)), dma((4,)), dma((1,)), dma((1,)), dma((4,)), dma((4,)),
        pltpu.SemaphoreType.REGULAR((2,)),
    ]
    return pl.pallas_call(
        functools.partial(kernel, cfg),
        out_shape=(
            jax.ShapeDtypeStruct((2, S, bl, lt), F32),
            jax.ShapeDtypeStruct((2 * STEPS, 8, 128), F32),
            jax.ShapeDtypeStruct((W, bl, nb), F32),
        ),
        in_specs=[hbm, hbm, hbm, vm],
        out_specs=(hbm, vm, hbm),
        scratch_shapes=scratch,
        compiler_params=pltpu.CompilerParams(collective_id=0, has_side_effects=True, vmem_limit_bytes=VM_LIMIT),
    )(l3, rbt, psi, wl)


def mpo_rows(mpo_two):
    w = mpo_two.reshape(W, W, S, S).transpose(0, 3, 2, 1)
    w = jnp.concatenate([w[..., :16].reshape(W * S, 64), w[..., 16:].reshape(W * S, 16)], axis=1)
    one = lax.reduce_precision(w, 8, 7)
    two = lax.reduce_precision(w - one, 8, 7)
    three = w - one - two
    none = jnp.zeros_like(w)
    left = jnp.concatenate([
        jnp.concatenate([one, one, one], 1),
        jnp.concatenate([two, two, none], 1),
        jnp.concatenate([three, none, none], 1)], 0)
    return jnp.pad(left, ((0, 0), (0, 16))).astype(BF)


def build(mesh, cfg):
    def lanczos(psi_block, left_env, right_env, mpo_two):
        lt, a, bl = cfg.lt, cfg.a, cfg.bl
        l3 = jnp.transpose(left_env, (1, 0, 2))
        rbt = jnp.transpose(right_env, (1, 2, 0))
        psi = psi_block.reshape(2, lt, S, bl).transpose(0, 2, 3, 1)
        wl = mpo_rows(mpo_two)
        vec, scal, _ = steps(cfg, l3, rbt, psi, wl)
        vec = vec.transpose(0, 3, 1, 2).reshape(psi_block.shape)
        return scal[:STEPS, 0, 0], scal[STEPS:, 0, 0], vec

    return jax.shard_map(
        lanczos,
        mesh=mesh,
        in_specs=(P('left', None, None, 'right'), P('left', None, None), P('right', None, None), P()),
        out_specs=(P(), P(), P('left', None, None, 'right')),
        check_vma=False,
    )


def solution(mesh):
    return build(mesh, Cfg())
```

```python
import functools

import jax
import jax.numpy as jnp
from jax import lax
from jax.experimental import pallas as pl
from jax.experimental.pallas import tpu as pltpu
from jax.sharding import PartitionSpec as P

STEPS = 4
W = 20
S = 4
BF = jnp.bfloat16
F32 = jnp.float32
VM_LIMIT = 67043328


class Cfg:
    def __init__(self, lt=256, bl=128):
        self.lt = lt
        self.a = 2 * lt
        self.bl = bl
        self.nb = 4 * bl
        self.kb = self.nb // 2
        self.groups = bl // 16
        self.rows = 4 * bl
        self.nl = max(lt // 128, 1)
        self.elems = float(4 * self.a * S * self.nb)


def split3(x):
    one = x.astype(BF)
    rest = x - one.astype(F32)
    two = rest.astype(BF)
    return one, two, (rest - two.astype(F32)).astype(BF)


def remote(src, dst, send_sem, recv_sem, right, left):
    return pltpu.make_async_remote_copy(
        src_ref=src, dst_ref=dst, send_sem=send_sem, recv_sem=recv_sem,
        device_id={'right': right, 'left': left}, device_id_type=pl.DeviceIdType.MESH)


def enter(me):
    barrier = pltpu.get_barrier_semaphore()

    @pl.loop(1, 16)
    def _(off):
        peer = lax.rem(me + off, 16)
        pl.semaphore_signal(barrier, 1, device_id={'right': peer // 4, 'left': lax.rem(peer, 4)},
                            device_id_type=pl.DeviceIdType.MESH)

    pl.semaphore_wait(barrier, 15)


def sum_copy(k, me, peer, slot, out_ref, in_ref, send_sem, recv_sem):
    return remote(out_ref.at[k], in_ref.at[k, slot], send_sem.at[k, peer], recv_sem.at[k, slot], peer // 4, lax.rem(peer, 4))


def sum_start(parts, k, me, *refs):
    out_ref, in_ref = refs[:2]
    for i, part in enumerate(parts):
        out_ref[k, 8 * i:8 * i + 8] = part
        in_ref[k, me, 8 * i:8 * i + 8] = part

    @pl.loop(1, 16)
    def _(off):
        sum_copy(k, me, lax.rem(me + off, 16), me, *refs).start()


def sum_end(k, me, *refs):
    @pl.loop(1, 16)
    def _(off):
        peer = lax.rem(me + off, 16)
        sum_copy(k, me, peer, peer, *refs).wait_recv()

    total = refs[1][k, 0]
    for i in range(1, 16):
        total = total + refs[1][k, i]

    @pl.loop(1, 16)
    def _(off):
        sum_copy(k, me, lax.rem(me + off, 16), me, *refs).wait_send()

    total = jnp.sum(total, axis=1, keepdims=True)
    return [jnp.broadcast_to(jnp.sum(total[8 * i:8 * i + 8], axis=0, keepdims=True), (8, 128)) for i in range(2)]


def fold(x):
    r, c = x.shape
    if c % 128 == 0:
        x = jnp.sum(x.reshape(r // 8, 8, c), axis=0)
        acc = x[:, :128]
        for i in range(1, c // 128):
            acc = acc + x[:, i * 128:(i + 1) * 128]
        return acc
    return jnp.full((8, 128), jnp.sum(x) / 1024.0, F32)


CH = 10


def kernel(cfg, l3, rbt, psi, wl, out_v, out_s, rtf,
           u2, rts, vgs, vg, qg, lb, sb, rb0, yb, xs, ob, vp, acc, cf, al, ars, arr,
           lsem, rcsem, qsem, ar_s, ar_r, rs_s, rs_r, ag_s, ag_r, rh_s, rh_r, ro_s, ro_r, rf_s, rf_r, credit):
    lt, bl, nb, kb, rows, groups = cfg.lt, cfg.bl, cfg.nb, cfg.kb, cfg.rows, cfg.groups
    nl, lw = cfg.nl, cfg.lt // cfg.nl
    me_r = lax.axis_index('right')
    me_l = lax.axis_index('left')
    me = me_r * 4 + me_l
    core = lax.rem(me_l, 2)
    chip = me_l // 2
    mate = chip * 2 + 1 - core
    across = (1 - chip) * 2 + core
    own = pl.ds(pl.multiple_of(me_r * bl, bl), bl)
    half = W // 2
    ub0 = lb.at[1, 0:S, 0:16 * W]
    ub1 = lb.at[1, S:2 * S, 0:16 * W]
    sums = (me, ars, arr, ar_s, ar_r)
    zero = jnp.zeros((8, 128), F32)
    trips = W // CH
    low = lax.broadcasted_iota(jnp.int32, (8, lt), 0) < 4

    def get_l(n):
        tile = lax.rem(n // trips, 8)
        h, who = tile // 4, lax.rem(tile, 4)
        to = lax.rem(chip + 1 - who // 2, 2) * 2 + lax.rem(core + 1 - lax.rem(who, 2), 2)
        col = pl.ds(pl.multiple_of((2 * to + h) * lt, lt), lt)
        slot = lax.rem(n, 2)
        return pltpu.make_async_copy(l3.at[pl.ds(lax.rem(n, trips) * CH, CH), :, col], lb.at[slot], lsem.at[slot])

    def ag_copy(h, off):
        peer = lax.rem(me_r + off, 4)
        return remote(qg.at[h, :, own, :], qg.at[h, :, own, :], ag_s.at[h, off], ag_r.at[h, me_r], peer, me_l)

    def ag_from(h, off):
        peer = lax.rem(me_r + off, 4)
        there = qg.at[h, :, pl.ds(pl.multiple_of(peer * bl, bl), bl), :]
        return remote(there, there, ag_s.at[h, off], ag_r.at[h, peer], peer, me_l)

    def coef(i, shape):
        one = cf[i, 0:1, 0:1]
        return jnp.broadcast_to(one, shape)

    def update(h, j):
        for off in range(1, 4):
            ag_from(h, off).wait_recv()
            ag_copy(h, off).wait_send()

        for s in range(S):
            vp[h, s] = vg[h, s, own, :]
        chunk = min(256, nb)

        @pl.loop(0, S * (nb // chunk))
        def _(i):
            s = i // (nb // chunk)
            at = pl.ds(pl.multiple_of(lax.rem(i, nb // chunk) * chunk, chunk), chunk)
            new = (qg[h, s, at, :] - coef(0, (chunk, lt)) * vg[h, s, at, :]) * coef(1, (chunk, lt))
            vg[h, s, at, :] = new
            for k, v in enumerate(split3(new)):
                vgs[k, s, at, :] = v

        @pl.when(j < STEPS - 1)
        def _():
            for off in range(1, 4):
                pl.semaphore_signal(credit.at[h], 1, device_id={'right': lax.rem(me_r + off, 4), 'left': me_l},
                                    device_id_type=pl.DeviceIdType.MESH)

    def w_tile(ub, quad, i):
        base = 80 * quad
        pair = base + 64 + 8 * (i // 2)
        parts = [ub[s, base + 16 * i:base + 16 * i + 16, :] for s in range(S)]
        for s in (0, 2):
            one, two = ub[s, pair:pair + 8, :], ub[s + 1, pair:pair + 8, :]
            if i % 2 == 0:
                parts.append(jnp.where(low, one, pltpu.roll(two, 4, 0)))
            else:
                parts.append(jnp.where(low, pltpu.roll(one, 4, 0), two))
        x = jnp.concatenate(parts, axis=0) * coef(3, (4 * W, lt))
        return jnp.concatenate([*split3(x), jnp.zeros((16, lt), BF)], axis=0)

    def w_finish(quad, g, h):
        even, odd = [], []
        for i in range(W // 2):
            v = [ob[b, 8 * i:8 * i + 8, :] for b in range(4)]
            for dst, b0 in ((even, 0), (even, 2)):
                dst.append(jnp.where(low, v[b0], pltpu.roll(v[b0 + 1], 4, 0)))
            for dst, b0 in ((odd, 0), (odd, 2)):
                dst.append(jnp.where(low, pltpu.roll(v[b0], 4, 0), v[b0 + 1]))
        at = pl.ds(pl.multiple_of(g * 64 + 16 * quad, 16), 16)
        col = pl.ds(pl.multiple_of(h * lt, lt), lt)
        for first, lst in ((0, even), (1, odd)):
            for i in range(W // 2):
                u2[2 * i + first, at, col] = jnp.concatenate(lst[2 * i:2 * i + 2], axis=0)

    def group(it, ub_new, ub_old, do_r=True, do_w=True):
        before = lax.rem(it + 2 * groups - 1, 2 * groups)
        gw, hw = lax.rem(before, groups), before // groups
        at = pl.ds(pl.multiple_of(lax.rem(it, groups) * (16 * W), 16 * W), 16 * W)
        for s in range(S):
            if do_r:
                total = None
                for k in range(3):
                    for i in range(3 - k):
                        term = jnp.dot(rts[i, at, :], vgs[k, s], preferred_element_type=F32)
                        total = term if total is None else total + term
                ub_new[s] = total
            if not do_w:
                continue
            for i in range(4):
                y = jnp.dot(wl[...], w_tile(ub_old, s, i), preferred_element_type=F32)
                ob[i] = (y[:4 * W] + y[4 * W:8 * W]) + y[8 * W:]
            w_finish(s, gw, hw)

    def l_trip(n):
        get_l(n).wait()
        get_l(n + 1).start()
        slot, l0 = lax.rem(n, 2), lax.rem(n, trips) * CH
        total = None
        for m in range(CH):
            left, right = split3(u2[l0 + m]), split3(lb[slot, m])
            for k in range(3):
                for i in range(3 - k):
                    term = jnp.dot(left[i], right[k], preferred_element_type=F32)
                    total = term if total is None else total + term
        acc[...] += total

    def rs_copy(k, h):
        dst = (rb0, xs.at[h], yb)[k]
        i = 1 + h if k == 1 else (0 if k == 0 else 3)
        return remote(sb.at[k], dst, rs_s.at[k], rs_r.at[i], me_r, across if k == 1 else mate)

    def part_of(i):
        return acc[:, i * lw:(i + 1) * lw]

    def send_on(n, j):
        h, who = n // 4, lax.rem(n, 4)

        @pl.when(who == 0)
        def _():
            for i in range(nl):
                sb[0, i] = part_of(i)
            rs_copy(0, h).start()

        @pl.when(who == 1)
        def _():
            rs_copy(0, h).wait_recv()
            for i in range(nl):
                sb[1, i] = part_of(i) + rb0[i]
            rs_copy(1, h).start()

        @pl.when(who == 2)
        def _():
            rs_copy(0, h).wait_send()
            for i in range(nl):
                sb[2, i] = part_of(i)
            rs_copy(2, h).start()

        @pl.when(who == 3)
        def _():
            finish(h, j)

    def finish(h, j):
        rs_copy(2, h).wait_recv()
        rs_copy(1, h).wait_recv()
        for i in range(nl):
            yb[i] = (part_of(i) + yb[i]) + xs[h, i]
        rs_copy(1, h).wait_send()
        rs_copy(2, h).wait_send()
        for t in range(S):
            w = jnp.concatenate([yb[i, pl.ds(t, bl, stride=4), :] for i in range(nl)], axis=1)
            q = w - coef(2, (bl, lt)) * vp[h, t]
            al[0:8] += fold(w * vg[h, t, own, :])
            al[8:16] += fold(q * q)
            qg[h, t, own, :] = q

        @pl.when((j < STEPS - 1) & (h == 0))
        def _():
            ag_start(0)

    def ag_start(h):
        pl.semaphore_wait(credit.at[h], 3)
        for off in range(1, 4):
            ag_copy(h, off).start()

    own_psi = pltpu.make_async_copy(psi, qg.at[:, :, own, :], qsem)
    own_psi.start()

    def get_r(i):
        stage = (ub0, ub1)[i % 2]
        return pltpu.make_async_copy(rtf.at[i], stage.at[0:2], rcsem.at[i % 2])

    lanes = nb // 2
    per = lanes // bl

    def columns(peer):
        return peer // per, pl.ds(pl.multiple_of(lax.rem(peer, per) * bl, bl), bl)

    def r_half(off, peer):
        to = lax.rem(me_r + off, 4)
        part = pl.ds(pl.multiple_of(core * (8 * W), 8 * W), 8 * W)
        e, col = columns(peer)
        return remote(rbt.at[pl.ds(to * groups, groups), part, :], rtf.at[:, e, part, col],
                      rh_s.at[off], rh_r.at[peer], to, me_l)

    def r_pass(off, which):
        e, col = columns(lax.rem(me_r + off, 4))
        part = rtf.at[:, e, pl.ds(pl.multiple_of(which * (8 * W), 8 * W), 8 * W), col]
        return remote(part, part, rf_s.at[off], rf_r.at[off], me_r, mate)

    def r_own():
        e, col = columns(me_r)
        return remote(rbt.at[pl.ds(me_r * groups, groups)], rtf.at[:, e, :, col], ro_s.at[0], ro_r.at[0], me_r, mate)

    enter(me)
    own_psi.wait()
    part = zero
    for h in range(2):
        for s in range(S):
            x = qg[h, s, own, :]
            part = part + fold(x * x)
    sum_start((part, zero), 2, *sums)
    for off in range(1, 4):
        r_half(off, me_r).start()
    r_own().start()
    for h in range(2):
        for off in range(1, 4):
            ag_copy(h, off).start()
    get_l(0).start()
    vg[...] = jnp.zeros(vg.shape, F32)
    norm = jnp.sqrt(sum_end(2, *sums)[0] / cfg.elems)
    cf[0] = zero
    cf[1] = 1.0 / norm
    cf[2] = zero
    cf[3] = zero + 1.0
    cf[4] = norm
    lowb = lax.broadcasted_iota(jnp.int32, (8, lanes), 0) < 4

    for off in range(1, 4):
        r_half(off, lax.rem(me_r + off, 4)).wait_recv()
        r_pass(off, core).start()
    r_own().wait_recv()
    for off in range(1, 4):
        r_pass(off, 1 - core).wait_recv()
    get_r(0).start()
    for i in range(groups):
        if i + 1 < groups:
            get_r(i + 1).start()
        get_r(i).wait()
        stage = (ub0, ub1)[i % 2]

        @pl.loop(0, 2)
        def _(e):
            raw = stage[e].reshape(W, 16, lanes)
            for b8 in range(2):
                cols = raw[:, 8 * b8:8 * b8 + 8]
                one = jnp.transpose(cols[0:8], (1, 0, 2))
                two = jnp.transpose(cols[8:16], (1, 0, 2))
                tail = jnp.transpose(jnp.concatenate([cols[16:20], cols[16:20]], axis=0), (1, 0, 2))
                for quad in range(2):
                    b0 = 4 * quad
                    parts = []
                    for b in range(b0, b0 + 4):
                        parts += [one[b], two[b]]
                    parts += [jnp.where(lowb, tail[b0], tail[b0 + 1]), jnp.where(lowb, tail[b0 + 2], tail[b0 + 3])]
                    row = i * 320 + 160 * b8 + 80 * quad
                    for k, v in enumerate(split3(jnp.concatenate(parts, axis=0))):
                        rts[k, row:row + 80, pl.ds(pl.multiple_of(e * lanes, lanes), lanes)] = v

    for off in range(1, 4):
        r_half(off, me_r).wait_send()
        r_pass(off, core).wait_send()
    r_own().wait_send()

    def norm_start():
        part = zero
        for h in range(2):
            for s in range(S):
                w = (qg[h, s, own, :] - coef(0, (bl, lt)) * vg[h, s, own, :]) * coef(1, (bl, lt))
                part = part + fold(w * w)
        sum_start((part, zero), 1, *sums)

    def norm_end(j):
        gamma = jnp.sqrt(sum_end(1, *sums)[0] / cfg.elems)
        beta = gamma * cf[4]
        out_s[STEPS + j] = beta
        cf[2] = beta * cf[3]
        cf[3] = 1.0 / gamma

    @pl.loop(0, STEPS)
    def _(j):
        update(0, j)
        group(0, ub0, ub1, do_w=False)

        @pl.when(j > 0)
        def _():
            norm_end(j - 1)

        group(1, ub1, ub0)

        @pl.loop(1, groups)
        def _(p):
            @pl.when(p == groups // 2)
            def _():
                update(1, j)

            group(2 * p, ub0, ub1)
            group(2 * p + 1, ub1, ub0)

        group(2 * groups, ub0, ub1, do_r=False)
        al[...] = jnp.zeros((16, 128), F32)
        acc[...] = jnp.zeros((rows, lt), F32)

        @pl.loop(0, 8 * trips)
        def _(n):
            l_trip(n)

            @pl.when(lax.rem(n, trips) == trips - 1)
            def _():
                send_on(n // trips, j)
                acc[...] = jnp.zeros((rows, lt), F32)

        sum_start((al[0:8], al[8:16]), 0, *sums)
        dot, square = sum_end(0, *sums)
        alpha = cf[3] * (dot / cfg.elems)
        size = jnp.sqrt(square / cfg.elems)
        size = jnp.where(size > 0.0, size, 1.0)
        out_s[j] = alpha
        cf[0] = alpha * cf[3]
        cf[1] = 1.0 / size
        cf[4] = size
        norm_start()

        @pl.when(j < STEPS - 1)
        def _():
            ag_start(1)

    norm_end(STEPS - 1)
    get_l(0).wait()
    for h in range(2):
        for s in range(S):
            v = (qg[h, s, own, :] - coef(0, (bl, lt)) * vg[h, s, own, :]) * coef(1, (bl, lt))
            qg[h, s, own, :] = v * coef(3, (bl, lt))
    result = pltpu.make_async_copy(qg.at[:, :, own, :], out_v, qsem)
    result.start()
    result.wait()


def steps(cfg, l3, rbt, psi, wl):
    lt, bl, nb, rows = cfg.lt, cfg.bl, cfg.nb, cfg.rows
    hbm = pl.BlockSpec(memory_space=pl.ANY)
    vm = pl.BlockSpec(memory_space=pltpu.VMEM)
    dma = pltpu.SemaphoreType.DMA
    block = (cfg.nl, rows, lt // cfg.nl)
    scratch = [
        pltpu.VMEM((W, rows, cfg.a), F32),
        pltpu.VMEM((3, W * bl, nb), BF),
        pltpu.VMEM((3, S, nb, lt), BF),
        pltpu.VMEM((2, S, nb, lt), F32),
        pltpu.VMEM((2, S, nb, lt), F32),
        pltpu.VMEM((2, CH, cfg.a, lt), F32),
        pltpu.VMEM((3, *block), F32),
        pltpu.VMEM(block, F32),
        pltpu.VMEM(block, F32),
        pltpu.VMEM((2, *block), F32),
        pltpu.VMEM((4, 4 * W, lt), F32),
        pltpu.VMEM((2, S, bl, lt), F32),
        pltpu.VMEM((rows, lt), F32),
        pltpu.VMEM((5, 8, 128), F32),
        pltpu.VMEM((16, 128), F32),
        pltpu.VMEM((3, 16, 128), F32),
        pltpu.VMEM((3, 16, 16, 128), F32),
        dma((2,)), dma((2,)), dma, dma((3, 16)), dma((3, 16)), dma((3,)), dma((4,)), dma((2, 4)), dma((2, 4)),
        dma((4,)), dma((4,)), dma((1,)), dma((1,)), dma((4,)), dma((4,)),
        pltpu.SemaphoreType.REGULAR((2,)),
    ]
    return pl.pallas_call(
        functools.partial(kernel, cfg),
        out_shape=(
            jax.ShapeDtypeStruct((2, S, bl, lt), F32),
            jax.ShapeDtypeStruct((2 * STEPS, 8, 128), F32),
            jax.ShapeDtypeStruct((cfg.groups, 2, 16 * W, nb // 2), F32),
        ),
        in_specs=[hbm, hbm, hbm, vm],
        out_specs=(hbm, vm, hbm),
        scratch_shapes=scratch,
        compiler_params=pltpu.CompilerParams(collective_id=0, has_side_effects=True, vmem_limit_bytes=VM_LIMIT),
    )(l3, rbt, psi, wl)


def mpo_rows(mpo_two):
    w = mpo_two.reshape(W, W, S, S).transpose(0, 3, 2, 1)
    w = jnp.concatenate([w[..., :16].reshape(W * S, 64), w[..., 16:].reshape(W * S, 16)], axis=1)
    one = lax.reduce_precision(w, 8, 7)
    two = lax.reduce_precision(w - one, 8, 7)
    three = w - one - two
    none = jnp.zeros_like(w)
    left = jnp.concatenate([
        jnp.concatenate([one, one, one], 1),
        jnp.concatenate([two, two, none], 1),
        jnp.concatenate([three, none, none], 1)], 0)
    return jnp.pad(left, ((0, 0), (0, 16))).astype(BF)


def build(mesh, cfg):
    def lanczos(psi_block, left_env, right_env, mpo_two):
        lt, a, bl = cfg.lt, cfg.a, cfg.bl
        l3 = jnp.transpose(left_env, (1, 0, 2))
        rbt = right_env.reshape(bl, W, 4 * cfg.groups, 16).transpose(2, 1, 3, 0).reshape(4 * cfg.groups, 16 * W, bl)
        psi = psi_block.reshape(2, lt, S, bl).transpose(0, 2, 3, 1)
        wl = mpo_rows(mpo_two)
        vec, scal, _ = steps(cfg, l3, rbt, psi, wl)
        vec = vec.transpose(0, 3, 1, 2).reshape(psi_block.shape)
        return scal[:STEPS, 0, 0], scal[STEPS:, 0, 0], vec

    return jax.shard_map(
        lanczos,
        mesh=mesh,
        in_specs=(P('left', None, None, 'right'), P('left', None, None), P('right', None, None), P()),
        out_specs=(P(), P(), P('left', None, None, 'right')),
        check_vma=False,
    )


def solution(mesh):
    return build(mesh, Cfg())
```

```python
import functools

import jax
import jax.numpy as jnp
from jax import lax
from jax.experimental import pallas as pl
from jax.experimental.pallas import tpu as pltpu
from jax.sharding import PartitionSpec as P

STEPS = 4
W = 20
S = 4
BF = jnp.bfloat16
F32 = jnp.float32
VM_LIMIT = 67043328


class Cfg:
    def __init__(self, lt=256, bl=128):
        self.lt = lt
        self.a = 2 * lt
        self.bl = bl
        self.nb = 4 * bl
        self.kb = self.nb // 2
        self.groups = bl // 16
        self.rows = 4 * bl
        self.nl = max(lt // 128, 1)
        self.elems = float(4 * self.a * S * self.nb)


def split3(x):
    one = x.astype(BF)
    rest = x - one.astype(F32)
    two = rest.astype(BF)
    return one, two, (rest - two.astype(F32)).astype(BF)


def remote(src, dst, send_sem, recv_sem, right, left):
    return pltpu.make_async_remote_copy(
        src_ref=src, dst_ref=dst, send_sem=send_sem, recv_sem=recv_sem,
        device_id={'right': right, 'left': left}, device_id_type=pl.DeviceIdType.MESH)


def enter(me):
    barrier = pltpu.get_barrier_semaphore()

    @pl.loop(1, 16)
    def _(off):
        peer = lax.rem(me + off, 16)
        pl.semaphore_signal(barrier, 1, device_id={'right': peer // 4, 'left': lax.rem(peer, 4)},
                            device_id_type=pl.DeviceIdType.MESH)


def sum_copy(k, me, peer, slot, out_ref, in_ref, send_sem, recv_sem):
    return remote(out_ref.at[k], in_ref.at[k, slot], send_sem.at[k, peer], recv_sem.at[k, slot], peer // 4, lax.rem(peer, 4))


def sum_start(parts, k, me, *refs):
    out_ref, in_ref = refs[:2]
    for i, part in enumerate(parts):
        out_ref[k, 8 * i:8 * i + 8] = part
        in_ref[k, me, 8 * i:8 * i + 8] = part

    @pl.loop(1, 16)
    def _(off):
        sum_copy(k, me, lax.rem(me + off, 16), me, *refs).start()


def sum_end(k, me, *refs):
    @pl.loop(1, 16)
    def _(off):
        peer = lax.rem(me + off, 16)
        sum_copy(k, me, peer, peer, *refs).wait_recv()

    total = refs[1][k, 0]
    for i in range(1, 16):
        total = total + refs[1][k, i]

    total = jnp.sum(total, axis=1, keepdims=True)
    return [jnp.broadcast_to(jnp.sum(total[8 * i:8 * i + 8], axis=0, keepdims=True), (8, 128)) for i in range(2)]


def sum_sent(k, me, *refs):
    @pl.loop(1, 16)
    def _(off):
        sum_copy(k, me, lax.rem(me + off, 16), me, *refs).wait_send()


def fold(x):
    r, c = x.shape
    if c % 128 == 0:
        x = jnp.sum(x.reshape(r // 8, 8, c), axis=0)
        acc = x[:, :128]
        for i in range(1, c // 128):
            acc = acc + x[:, i * 128:(i + 1) * 128]
        return acc
    return jnp.full((8, 128), jnp.sum(x) / 1024.0, F32)


CH = 10


def kernel(cfg, l3, rb3, psi, wl, out_v, out_s,
           u2, rts, vgs, vg, qg, lb, sb, rb0, yb, xs, ob, vp, acc, cf, al, ars, arr,
           lsem, psem, qsem, ar_s, ar_r, rs_s, rs_r, ag_s, ag_r, rh_s, rh_r, rx_s, rx_r, rm_s, rm_r, rn_s, rn_r, credit):
    lt, bl, nb, kb, rows, groups = cfg.lt, cfg.bl, cfg.nb, cfg.kb, cfg.rows, cfg.groups
    nl, lw = cfg.nl, cfg.lt // cfg.nl
    me_r = lax.axis_index('right')
    me_l = lax.axis_index('left')
    me = me_r * 4 + me_l
    core = lax.rem(me_l, 2)
    chip = me_l // 2
    mate = chip * 2 + 1 - core
    across = (1 - chip) * 2 + core
    own = pl.ds(pl.multiple_of(me_r * bl, bl), bl)
    ub0 = lb.at[1, 0:S, 0:16 * W]
    ub1 = lb.at[1, S:2 * S, 0:16 * W]
    sums = (me, ars, arr, ar_s, ar_r)
    zero = jnp.zeros((8, 128), F32)
    trips = W // CH
    low = lax.broadcasted_iota(jnp.int32, (8, lt), 0) < 4

    def get_l(n):
        tile = lax.rem(n // trips, 8)
        h, who = tile // 4, lax.rem(tile, 4)
        to = lax.rem(chip + 1 - who // 2, 2) * 2 + lax.rem(core + 1 - lax.rem(who, 2), 2)
        col = pl.ds(pl.multiple_of((2 * to + h) * lt, lt), lt)
        slot = lax.rem(n, 2)
        return pltpu.make_async_copy(l3.at[pl.ds(lax.rem(n, trips) * CH, CH), :, col], lb.at[slot], lsem.at[slot])

    def ag_copy(h, off):
        peer = lax.rem(me_r + off, 4)
        return remote(qg.at[h, :, own, :], qg.at[h, :, own, :], ag_s.at[h, off], ag_r.at[h, me_r], peer, me_l)

    def ag_from(h, off):
        peer = lax.rem(me_r + off, 4)
        there = qg.at[h, :, pl.ds(pl.multiple_of(peer * bl, bl), bl), :]
        return remote(there, there, ag_s.at[h, off], ag_r.at[h, peer], peer, me_l)

    def coef(i, shape):
        one = cf[i, 0:1, 0:1]
        return jnp.broadcast_to(one, shape)

    def update(h, j):
        for off in range(1, 4):
            ag_from(h, off).wait_recv()
            ag_copy(h, off).wait_send()

        for s in range(S):
            vp[h, s] = vg[h, s, own, :]
        chunk = min(256, nb)

        @pl.loop(0, S * (nb // chunk))
        def _(i):
            s = i // (nb // chunk)
            at = pl.ds(pl.multiple_of(lax.rem(i, nb // chunk) * chunk, chunk), chunk)
            new = (qg[h, s, at, :] - coef(0, (chunk, lt)) * vg[h, s, at, :]) * coef(1, (chunk, lt))
            vg[h, s, at, :] = new
            for k, v in enumerate(split3(new)):
                vgs[k, s, at, :] = v

        @pl.when(j < STEPS - 1)
        def _():
            for off in range(1, 4):
                pl.semaphore_signal(credit.at[h], 1, device_id={'right': lax.rem(me_r + off, 4), 'left': me_l},
                                    device_id_type=pl.DeviceIdType.MESH)

    def w_tile(ub, quad, i):
        base = 80 * quad
        pair = base + 64 + 8 * (i // 2)
        parts = [ub[s, base + 16 * i:base + 16 * i + 16, :] for s in range(S)]
        for s in (0, 2):
            one, two = ub[s, pair:pair + 8, :], ub[s + 1, pair:pair + 8, :]
            if i % 2 == 0:
                parts.append(jnp.where(low, one, pltpu.roll(two, 4, 0)))
            else:
                parts.append(jnp.where(low, pltpu.roll(one, 4, 0), two))
        x = jnp.concatenate(parts, axis=0) * coef(3, (4 * W, lt))
        return jnp.concatenate([*split3(x), jnp.zeros((16, lt), BF)], axis=0)

    def w_finish(quad, g, h):
        even, odd = [], []
        for i in range(W // 2):
            v = [ob[b, 8 * i:8 * i + 8, :] for b in range(4)]
            for dst, b0 in ((even, 0), (even, 2)):
                dst.append(jnp.where(low, v[b0], pltpu.roll(v[b0 + 1], 4, 0)))
            for dst, b0 in ((odd, 0), (odd, 2)):
                dst.append(jnp.where(low, pltpu.roll(v[b0], 4, 0), v[b0 + 1]))
        at = pl.ds(pl.multiple_of(g * 64 + 16 * quad, 16), 16)
        col = pl.ds(pl.multiple_of(h * lt, lt), lt)
        for first, lst in ((0, even), (1, odd)):
            for i in range(W // 2):
                u2[2 * i + first, at, col] = jnp.concatenate(lst[2 * i:2 * i + 2], axis=0)

    def group(it, ub_new, ub_old, do_r=True, do_w=True):
        before = lax.rem(it + 2 * groups - 1, 2 * groups)
        gw, hw = lax.rem(before, groups), before // groups
        at = pl.ds(pl.multiple_of(lax.rem(it, groups) * (16 * W), 16 * W), 16 * W)
        for s in range(S):
            if do_r:
                total = None
                for k in range(3):
                    for i in range(3 - k):
                        term = jnp.dot(rts[i, at, :], vgs[k, s], preferred_element_type=F32)
                        total = term if total is None else total + term
                ub_new[s] = total
            if not do_w:
                continue
            for i in range(4):
                y = jnp.dot(wl[...], w_tile(ub_old, s, i), preferred_element_type=F32)
                ob[i] = (y[:4 * W] + y[4 * W:8 * W]) + y[8 * W:]
            w_finish(s, gw, hw)

    def l_trip(n):
        get_l(n).wait()
        get_l(n + 1).start()
        slot, l0 = lax.rem(n, 2), lax.rem(n, trips) * CH
        total = None
        for m in range(CH):
            left, right = split3(u2[l0 + m]), split3(lb[slot, m])
            for k in range(3):
                for i in range(3 - k):
                    term = jnp.dot(left[i], right[k], preferred_element_type=F32)
                    total = term if total is None else total + term
        acc[...] += total

    def rs_copy(k, h):
        dst = (rb0, xs.at[h], yb)[k]
        i = 1 + h if k == 1 else (0 if k == 0 else 3)
        return remote(sb.at[k], dst, rs_s.at[k], rs_r.at[i], me_r, across if k == 1 else mate)

    def part_of(i):
        return acc[:, i * lw:(i + 1) * lw]

    def send_on(n, j):
        h, who = n // 4, lax.rem(n, 4)

        @pl.when(who == 0)
        def _():
            for i in range(nl):
                sb[0, i] = part_of(i)
            rs_copy(0, h).start()

        @pl.when(who == 1)
        def _():
            rs_copy(0, h).wait_recv()
            for i in range(nl):
                sb[1, i] = part_of(i) + rb0[i]
            rs_copy(1, h).start()

        @pl.when(who == 2)
        def _():
            rs_copy(0, h).wait_send()
            for i in range(nl):
                sb[2, i] = part_of(i)
            rs_copy(2, h).start()

        @pl.when(who == 3)
        def _():
            finish(h, j)

    def finish(h, j):
        rs_copy(2, h).wait_recv()
        rs_copy(1, h).wait_recv()
        for i in range(nl):
            yb[i] = (part_of(i) + yb[i]) + xs[h, i]
        rs_copy(1, h).wait_send()
        rs_copy(2, h).wait_send()
        for t in range(S):
            w = jnp.concatenate([yb[i, pl.ds(t, bl, stride=4), :] for i in range(nl)], axis=1)
            q = w - coef(2, (bl, lt)) * vp[h, t]
            al[0:8] += fold(w * vg[h, t, own, :])
            al[8:16] += fold(q * q)
            qg[h, t, own, :] = q

        @pl.when((j < STEPS - 1) & (h == 0))
        def _():
            ag_start(0)

    def ag_start(h):
        pl.semaphore_wait(credit.at[h], 3)
        for off in range(1, 4):
            ag_copy(h, off).start()

    def get_psi(i):
        return pltpu.make_async_copy(psi.at[i], sb.at[i // 2, i % 2], psem.at[i])

    load_r = pltpu.make_async_copy(rb3, u2.at[:, 0:bl, :], qsem)
    load_r.start()
    for i in range(4):
        get_psi(i).start()
    enter(me)
    part = zero
    for i in range(4):
        get_psi(i).wait()
        for s in range(S):
            x = sb[i // 2, i % 2, pl.ds(s, bl, stride=S), :]
            part = part + fold(x * x)
            qg[i // 2, s, own, (i % 2) * lw:(i % 2 + 1) * lw] = x.T
    load_r.wait()
    block = 16 * W

    @pl.loop(0, W)
    def _(r):
        at = pl.ds(pl.multiple_of(bl + r * 16, 16), 16)
        turned = [u2[r, 0:bl, p * bl:(p + 1) * bl].T for p in range(4)]
        for p, x in enumerate(turned):
            for g in range(groups):
                u2[g, at, p * bl:(p + 1) * bl] = x[16 * g:16 * g + 16]

    def to_send(peer, q):
        return u2.at[0:groups, pl.ds(pl.multiple_of(bl + q * (block // 4), 8), block // 4),
                     pl.ds(pl.multiple_of(peer * bl, bl), bl)]

    def landed(peer, q):
        return u2.at[groups:2 * groups, pl.ds(pl.multiple_of(bl + q * (block // 4), 8), block // 4),
                     pl.ds(pl.multiple_of(peer * bl, bl), bl)]

    def r_quarter(off, peer):
        to = lax.rem(me_r + off, 4)
        return remote(to_send(to, me_l), landed(peer, me_l), rh_s.at[off], rh_r.at[peer], to, me_l)

    def pass_on(off, q, where, send_sem, recv_sem):
        part = landed(lax.rem(me_r + off, 4), q)
        return remote(part, part, send_sem.at[off], recv_sem.at[off], me_r, where)

    pl.semaphore_wait(pltpu.get_barrier_semaphore(), 15)
    sum_start((part, zero), 2, *sums)
    for off in range(1, 4):
        r_quarter(off, me_r).start()
    for h in range(2):
        for off in range(1, 4):
            ag_copy(h, off).start()
    get_l(0).start()

    @pl.loop(0, groups)
    def _(g):
        col = pl.ds(pl.multiple_of(me_r * bl, bl), bl)
        u2[groups + g, bl:bl + block, col] = u2[g, bl:bl + block, col]

    vg[...] = jnp.zeros(vg.shape, F32)
    norm = jnp.sqrt(sum_end(2, *sums)[0] / cfg.elems)
    cf[0] = zero
    cf[1] = 1.0 / norm
    cf[2] = zero
    cf[3] = zero + 1.0
    cf[4] = norm
    sum_sent(2, *sums)
    diag = (1 - chip) * 2 + 1 - core
    for off in range(1, 4):
        r_quarter(off, lax.rem(me_r + off, 4)).wait_recv()
        pass_on(off, me_l, across, rx_s, rx_r).start()
        pass_on(off, me_l, mate, rm_s, rm_r).start()
    for off in range(1, 4):
        pass_on(off, across, across, rx_s, rx_r).wait_recv()
        pass_on(off, across, mate, rn_s, rn_r).start()
    for off in range(1, 4):
        pass_on(off, mate, mate, rm_s, rm_r).wait_recv()
        pass_on(off, diag, mate, rn_s, rn_r).wait_recv()
    lanes = nb // 2
    lowb = lax.broadcasted_iota(jnp.int32, (8, lanes), 0) < 4

    @pl.loop(0, groups)
    def _(g):
        for e in range(2):
            raw = u2[groups + g, bl:bl + block, e * lanes:(e + 1) * lanes].reshape(W, 16, lanes)
            for b8 in range(2):
                cols = raw[:, 8 * b8:8 * b8 + 8]
                one = jnp.transpose(cols[0:8], (1, 0, 2))
                two = jnp.transpose(cols[8:16], (1, 0, 2))
                tail = jnp.transpose(jnp.concatenate([cols[16:20], cols[16:20]], axis=0), (1, 0, 2))
                for quad in range(2):
                    b0 = 4 * quad
                    parts = []
                    for b in range(b0, b0 + 4):
                        parts += [one[b], two[b]]
                    parts += [jnp.where(lowb, tail[b0], tail[b0 + 1]), jnp.where(lowb, tail[b0 + 2], tail[b0 + 3])]
                    at = pl.ds(pl.multiple_of(g * block + 160 * b8 + 80 * quad, 16), 80)
                    for k, v in enumerate(split3(jnp.concatenate(parts, axis=0))):
                        rts[k, at, e * lanes:(e + 1) * lanes] = v

    for off in range(1, 4):
        r_quarter(off, me_r).wait_send()
        pass_on(off, me_l, across, rx_s, rx_r).wait_send()
        pass_on(off, me_l, mate, rm_s, rm_r).wait_send()
        pass_on(off, across, mate, rn_s, rn_r).wait_send()

    def norm_start():
        part = zero
        for h in range(2):
            for s in range(S):
                w = (qg[h, s, own, :] - coef(0, (bl, lt)) * vg[h, s, own, :]) * coef(1, (bl, lt))
                part = part + fold(w * w)
        sum_start((part, zero), 1, *sums)

    def norm_end(j):
        gamma = jnp.sqrt(sum_end(1, *sums)[0] / cfg.elems)
        beta = gamma * cf[4]
        out_s[STEPS + j] = beta
        cf[2] = beta * cf[3]
        cf[3] = 1.0 / gamma
        sum_sent(1, *sums)

    @pl.loop(0, STEPS)
    def _(j):
        update(0, j)
        group(0, ub0, ub1, do_w=False)

        @pl.when(j > 0)
        def _():
            norm_end(j - 1)

        group(1, ub1, ub0)

        @pl.loop(1, groups)
        def _(p):
            @pl.when(p == groups // 2)
            def _():
                update(1, j)

            group(2 * p, ub0, ub1)
            group(2 * p + 1, ub1, ub0)

        group(2 * groups, ub0, ub1, do_r=False)
        al[...] = jnp.zeros((16, 128), F32)
        acc[...] = jnp.zeros((rows, lt), F32)

        @pl.loop(0, 8 * trips)
        def _(n):
            l_trip(n)

            @pl.when(lax.rem(n, trips) == trips - 1)
            def _():
                send_on(n // trips, j)
                acc[...] = jnp.zeros((rows, lt), F32)

        sum_start((al[0:8], al[8:16]), 0, *sums)
        dot, square = sum_end(0, *sums)
        alpha = cf[3] * (dot / cfg.elems)
        size = jnp.sqrt(square / cfg.elems)
        size = jnp.where(size > 0.0, size, 1.0)
        out_s[j] = alpha
        cf[0] = alpha * cf[3]
        cf[1] = 1.0 / size
        cf[4] = size
        norm_start()

        @pl.when(j < STEPS - 1)
        def _():
            ag_start(1)

        sum_sent(0, *sums)

    norm_end(STEPS - 1)
    get_l(0).wait()
    for h in range(2):
        for s in range(S):
            v = (qg[h, s, own, :] - coef(0, (bl, lt)) * vg[h, s, own, :]) * coef(1, (bl, lt))
            qg[h, s, own, :] = v * coef(3, (bl, lt))
    result = pltpu.make_async_copy(qg.at[:, :, own, :], out_v, qsem)
    result.start()
    result.wait()


def steps(cfg, l3, rb3, psi, wl):
    lt, bl, nb, rows = cfg.lt, cfg.bl, cfg.nb, cfg.rows
    hbm = pl.BlockSpec(memory_space=pl.ANY)
    vm = pl.BlockSpec(memory_space=pltpu.VMEM)
    dma = pltpu.SemaphoreType.DMA
    block = (cfg.nl, rows, lt // cfg.nl)
    scratch = [
        pltpu.VMEM((W, rows, cfg.a), F32),
        pltpu.VMEM((3, W * bl, nb), BF),
        pltpu.VMEM((3, S, nb, lt), BF),
        pltpu.VMEM((2, S, nb, lt), F32),
        pltpu.VMEM((2, S, nb, lt), F32),
        pltpu.VMEM((2, CH, cfg.a, lt), F32),
        pltpu.VMEM((3, *block), F32),
        pltpu.VMEM(block, F32),
        pltpu.VMEM(block, F32),
        pltpu.VMEM((2, *block), F32),
        pltpu.VMEM((4, 4 * W, lt), F32),
        pltpu.VMEM((2, S, bl, lt), F32),
        pltpu.VMEM((rows, lt), F32),
        pltpu.VMEM((5, 8, 128), F32),
        pltpu.VMEM((16, 128), F32),
        pltpu.VMEM((3, 16, 128), F32),
        pltpu.VMEM((3, 16, 16, 128), F32),
        dma((2,)), dma((4,)), dma, dma((3, 16)), dma((3, 16)), dma((3,)), dma((4,)), dma((2, 4)), dma((2, 4)),
        dma((4,)), dma((4,)), dma((4,)), dma((4,)), dma((4,)), dma((4,)), dma((4,)), dma((4,)),
        pltpu.SemaphoreType.REGULAR((2,)),
    ]
    return pl.pallas_call(
        functools.partial(kernel, cfg),
        out_shape=(
            jax.ShapeDtypeStruct((2, S, bl, lt), F32),
            jax.ShapeDtypeStruct((2 * STEPS, 8, 128), F32),
        ),
        in_specs=[hbm, hbm, hbm, vm],
        out_specs=(hbm, vm),
        scratch_shapes=scratch,
        compiler_params=pltpu.CompilerParams(collective_id=0, has_side_effects=True, vmem_limit_bytes=VM_LIMIT),
    )(l3, rb3, psi, wl)


def mpo_rows(mpo_two):
    w = mpo_two.reshape(W, W, S, S).transpose(0, 3, 2, 1)
    w = jnp.concatenate([w[..., :16].reshape(W * S, 64), w[..., 16:].reshape(W * S, 16)], axis=1)
    one = lax.reduce_precision(w, 8, 7)
    two = lax.reduce_precision(w - one, 8, 7)
    three = w - one - two
    none = jnp.zeros_like(w)
    left = jnp.concatenate([
        jnp.concatenate([one, one, one], 1),
        jnp.concatenate([two, two, none], 1),
        jnp.concatenate([three, none, none], 1)], 0)
    return jnp.pad(left, ((0, 0), (0, 16))).astype(BF)


def build(mesh, cfg):
    def lanczos(psi_block, left_env, right_env, mpo_two):
        lt, a, bl = cfg.lt, cfg.a, cfg.bl
        l3 = jnp.transpose(left_env, (1, 0, 2))
        rb3 = jnp.transpose(right_env, (1, 0, 2))
        psi = psi_block.reshape(4, a, bl)
        wl = mpo_rows(mpo_two)
        vec, scal = steps(cfg, l3, rb3, psi, wl)
        vec = vec.transpose(0, 3, 1, 2).reshape(psi_block.shape)
        return scal[:STEPS, 0, 0], scal[STEPS:, 0, 0], vec

    return jax.shard_map(
        lanczos,
        mesh=mesh,
        in_specs=(P('left', None, None, 'right'), P('left', None, None), P('right', None, None), P()),
        out_specs=(P(), P(), P('left', None, None, 'right')),
        check_vma=False,
    )


def solution(mesh):
    return build(mesh, Cfg())
```

```python
import functools

import jax
import jax.numpy as jnp
from jax import lax
from jax.experimental import pallas as pl
from jax.experimental.pallas import tpu as pltpu
from jax.sharding import PartitionSpec as P

STEPS = 4
W = 20
S = 4
BF = jnp.bfloat16
F32 = jnp.float32
VM_LIMIT = 67043328


class Cfg:
    def __init__(self, lt=256, bl=128):
        self.lt = lt
        self.a = 2 * lt
        self.bl = bl
        self.nb = 4 * bl
        self.kb = self.nb // 2
        self.groups = bl // 16
        self.rows = 4 * bl
        self.nl = max(lt // 128, 1)
        self.elems = float(4 * self.a * S * self.nb)


def split3(x):
    one = x.astype(BF)
    rest = x - one.astype(F32)
    two = rest.astype(BF)
    return one, two, (rest - two.astype(F32)).astype(BF)


def remote(src, dst, send_sem, recv_sem, right, left):
    return pltpu.make_async_remote_copy(
        src_ref=src, dst_ref=dst, send_sem=send_sem, recv_sem=recv_sem,
        device_id={'right': right, 'left': left}, device_id_type=pl.DeviceIdType.MESH)


def enter(me):
    barrier = pltpu.get_barrier_semaphore()

    @pl.loop(1, 16)
    def _(off):
        peer = lax.rem(me + off, 16)
        pl.semaphore_signal(barrier, 1, device_id={'right': peer // 4, 'left': lax.rem(peer, 4)},
                            device_id_type=pl.DeviceIdType.MESH)


def sum_copy(k, me, peer, slot, out_ref, in_ref, send_sem, recv_sem):
    return remote(out_ref.at[k], in_ref.at[k, slot], send_sem.at[k, peer], recv_sem.at[k, slot], peer // 4, lax.rem(peer, 4))


def sum_start(parts, k, me, *refs):
    out_ref, in_ref = refs[:2]
    for i, part in enumerate(parts):
        out_ref[k, 8 * i:8 * i + 8] = part
        in_ref[k, me, 8 * i:8 * i + 8] = part

    @pl.loop(1, 16)
    def _(off):
        sum_copy(k, me, lax.rem(me + off, 16), me, *refs).start()


def sum_end(k, me, *refs):
    @pl.loop(1, 16)
    def _(off):
        peer = lax.rem(me + off, 16)
        sum_copy(k, me, peer, peer, *refs).wait_recv()

    total = refs[1][k, 0]
    for i in range(1, 16):
        total = total + refs[1][k, i]

    total = jnp.sum(total, axis=1, keepdims=True)
    return [jnp.broadcast_to(jnp.sum(total[8 * i:8 * i + 8], axis=0, keepdims=True), (8, 128)) for i in range(2)]


def sum_sent(k, me, *refs):
    @pl.loop(1, 16)
    def _(off):
        sum_copy(k, me, lax.rem(me + off, 16), me, *refs).wait_send()


def fold(x):
    r, c = x.shape
    if c % 128 == 0:
        x = jnp.sum(x.reshape(r // 8, 8, c), axis=0)
        acc = x[:, :128]
        for i in range(1, c // 128):
            acc = acc + x[:, i * 128:(i + 1) * 128]
        return acc
    return jnp.full((8, 128), jnp.sum(x) / 1024.0, F32)


CH = 10


def kernel(cfg, l3, rb3, psi, wl, out_v, out_s,
           u2, rts, vgs, vg, qg, lb, sb, rb0, yb, xs, ob, vp, acc, cf, al, ars, arr,
           lsem, psem, qsem, ar_s, ar_r, rs_s, rs_r, ag_s, ag_r, rh_s, rh_r, rx_s, rx_r, rm_s, rm_r, rn_s, rn_r, credit):
    lt, bl, nb, kb, rows, groups = cfg.lt, cfg.bl, cfg.nb, cfg.kb, cfg.rows, cfg.groups
    nl, lw = cfg.nl, cfg.lt // cfg.nl
    me_r = lax.axis_index('right')
    me_l = lax.axis_index('left')
    me = me_r * 4 + me_l
    core = lax.rem(me_l, 2)
    chip = me_l // 2
    mate = chip * 2 + 1 - core
    across = (1 - chip) * 2 + core
    diag = (1 - chip) * 2 + 1 - core
    peers = (me_r, me_r + 1 - 2 * lax.rem(me_r, 2), lax.rem(me_r + 2, 4), 3 - me_r)
    own = pl.ds(pl.multiple_of(me_r * bl, bl), bl)
    ub0 = lb.at[1, 0:S, 0:16 * W]
    ub1 = lb.at[1, S:2 * S, 0:16 * W]
    sums = (me, ars, arr, ar_s, ar_r)
    zero = jnp.zeros((8, 128), F32)
    trips = W // CH
    low = lax.broadcasted_iota(jnp.int32, (8, lt), 0) < 4

    def get_l(n):
        tile = lax.rem(n // trips, 8)
        h, who = tile // 4, lax.rem(tile, 4)
        to = lax.rem(chip + 1 - who // 2, 2) * 2 + lax.rem(core + 1 - lax.rem(who, 2), 2)
        col = pl.ds(pl.multiple_of((2 * to + h) * lt, lt), lt)
        slot = lax.rem(n, 2)
        return pltpu.make_async_copy(l3.at[pl.ds(lax.rem(n, trips) * CH, CH), :, col], lb.at[slot], lsem.at[slot])

    def ag_copy(h, k):
        return remote(qg.at[h, :, own, :], qg.at[h, :, own, :], ag_s.at[h, k], ag_r.at[h, k], peers[k], me_l)

    def ag_from(h, k):
        there = qg.at[h, :, pl.ds(pl.multiple_of(peers[k] * bl, bl), bl), :]
        return remote(there, there, ag_s.at[h, k], ag_r.at[h, k], peers[k], me_l)

    def coef(i, shape):
        one = cf[i, 0:1, 0:1]
        return jnp.broadcast_to(one, shape)

    def update(h, j):
        for off in range(1, 4):
            ag_from(h, off).wait_recv()
            ag_copy(h, off).wait_send()

        for s in range(S):
            vp[h, s] = vg[h, s, own, :]
        chunk = min(128, nb)

        @pl.loop(0, S * (nb // chunk))
        def _(i):
            s = i // (nb // chunk)
            at = pl.ds(pl.multiple_of(lax.rem(i, nb // chunk) * chunk, chunk), chunk)
            new = (qg[h, s, at, :] - coef(0, (chunk, lt)) * vg[h, s, at, :]) * coef(1, (chunk, lt))
            vg[h, s, at, :] = new
            for k, v in enumerate(split3(new)):
                vgs[k, s, at, :] = v

        @pl.when(j < STEPS - 1)
        def _():
            for off in range(1, 4):
                pl.semaphore_signal(credit.at[h], 1, device_id={'right': peers[off], 'left': me_l},
                                    device_id_type=pl.DeviceIdType.MESH)

    def w_tile(ub, quad, i):
        base = 80 * quad
        pair = base + 64 + 8 * (i // 2)
        parts = [ub[s, base + 16 * i:base + 16 * i + 16, :] for s in range(S)]
        for s in (0, 2):
            one, two = ub[s, pair:pair + 8, :], ub[s + 1, pair:pair + 8, :]
            if i % 2 == 0:
                parts.append(jnp.where(low, one, pltpu.roll(two, 4, 0)))
            else:
                parts.append(jnp.where(low, pltpu.roll(one, 4, 0), two))
        x = jnp.concatenate(parts, axis=0) * coef(3, (4 * W, lt))
        return jnp.concatenate([*split3(x), jnp.zeros((16, lt), BF)], axis=0)

    def w_finish(quad, g, h):
        even, odd = [], []
        for i in range(W // 2):
            v = [ob[b, 8 * i:8 * i + 8, :] for b in range(4)]
            for dst, b0 in ((even, 0), (even, 2)):
                dst.append(jnp.where(low, v[b0], pltpu.roll(v[b0 + 1], 4, 0)))
            for dst, b0 in ((odd, 0), (odd, 2)):
                dst.append(jnp.where(low, pltpu.roll(v[b0], 4, 0), v[b0 + 1]))
        at = pl.ds(pl.multiple_of(g * 64 + 16 * quad, 16), 16)
        col = pl.ds(pl.multiple_of(h * lt, lt), lt)
        for first, lst in ((0, even), (1, odd)):
            for i in range(W // 2):
                u2[2 * i + first, at, col] = jnp.concatenate(lst[2 * i:2 * i + 2], axis=0)

    def group(it, ub_new, ub_old, do_r=True, do_w=True):
        before = lax.rem(it + 2 * groups - 1, 2 * groups)
        gw, hw = lax.rem(before, groups), before // groups
        at = pl.ds(pl.multiple_of(lax.rem(it, groups) * (16 * W), 16 * W), 16 * W)
        for s in range(S):
            if do_r:
                total = None
                for k in range(3):
                    for i in range(3 - k):
                        term = jnp.dot(rts[i, at, :], vgs[k, s], preferred_element_type=F32)
                        total = term if total is None else total + term
                ub_new[s] = total
            if not do_w:
                continue
            for i in range(4):
                y = jnp.dot(wl[...], w_tile(ub_old, s, i), preferred_element_type=F32)
                ob[i] = (y[:4 * W] + y[4 * W:8 * W]) + y[8 * W:]
            w_finish(s, gw, hw)

    def l_trip(n):
        get_l(n).wait()
        get_l(n + 1).start()
        slot, l0 = lax.rem(n, 2), lax.rem(n, trips) * CH
        total = None
        for m in range(CH):
            left, right = split3(u2[l0 + m]), split3(lb[slot, m])
            for k in range(3):
                for i in range(3 - k):
                    term = jnp.dot(left[i], right[k], preferred_element_type=F32)
                    total = term if total is None else total + term
        acc[...] += total

    def rs_copy(k, h):
        dst = (rb0, xs.at[h], yb)[k]
        i = 1 + h if k == 1 else (0 if k == 0 else 3)
        return remote(sb.at[k], dst, rs_s.at[k], rs_r.at[i], me_r, across if k == 1 else mate)

    def part_of(i):
        return acc[:, i * lw:(i + 1) * lw]

    def send_on(n, j):
        h, who = n // 4, lax.rem(n, 4)

        @pl.when(who == 0)
        def _():
            for i in range(nl):
                sb[0, i] = part_of(i)
            rs_copy(0, h).start()

        @pl.when(who == 1)
        def _():
            rs_copy(0, h).wait_recv()
            for i in range(nl):
                sb[1, i] = part_of(i) + rb0[i]
            rs_copy(1, h).start()

        @pl.when(who == 2)
        def _():
            rs_copy(0, h).wait_send()
            for i in range(nl):
                sb[2, i] = part_of(i)
            rs_copy(2, h).start()

        @pl.when(who == 3)
        def _():
            finish(h, j)

    def finish(h, j):
        rs_copy(2, h).wait_recv()
        rs_copy(1, h).wait_recv()
        for i in range(nl):
            yb[i] = (part_of(i) + yb[i]) + xs[h, i]
        rs_copy(1, h).wait_send()
        rs_copy(2, h).wait_send()
        for t in range(S):
            w = jnp.concatenate([yb[i, pl.ds(t, bl, stride=4), :] for i in range(nl)], axis=1)
            q = w - coef(2, (bl, lt)) * vp[h, t]
            al[0:8] += fold(w * vg[h, t, own, :])
            al[8:16] += fold(q * q)
            qg[h, t, own, :] = q

        @pl.when((j < STEPS - 1) & (h == 0))
        def _():
            ag_start(0)

    def ag_start(h):
        pl.semaphore_wait(credit.at[h], 3)
        for off in range(1, 4):
            ag_copy(h, off).start()

    def get_psi(i):
        return pltpu.make_async_copy(psi.at[i], sb.at[i // 2, i % 2], psem.at[i])

    load_r = pltpu.make_async_copy(rb3, u2.at[:, 0:bl, :], qsem)
    load_r.start()
    for i in range(4):
        get_psi(i).start()
    enter(me)
    part = zero
    for i in range(4):
        get_psi(i).wait()
        for s in range(S):
            x = sb[i // 2, i % 2, pl.ds(s, bl, stride=S), :]
            part = part + fold(x * x)
            qg[i // 2, s, own, (i % 2) * lw:(i % 2 + 1) * lw] = x.T
    load_r.wait()
    block = 16 * W

    @pl.loop(0, W)
    def _(r):
        at = pl.ds(pl.multiple_of(bl + r * 16, 16), 16)
        turned = [u2[r, 0:bl, p * bl:(p + 1) * bl].T for p in range(4)]
        for p, x in enumerate(turned):
            for g in range(groups):
                u2[g, at, p * bl:(p + 1) * bl] = x[16 * g:16 * g + 16]

    def to_send(peer, q):
        return u2.at[0:groups, pl.ds(pl.multiple_of(bl + q * (block // 4), 8), block // 4),
                     pl.ds(pl.multiple_of(peer * bl, bl), bl)]

    def landed(peer, q):
        return u2.at[groups:2 * groups, pl.ds(pl.multiple_of(bl + q * (block // 4), 8), block // 4),
                     pl.ds(pl.multiple_of(peer * bl, bl), bl)]

    def r_quarter(k, peer):
        return remote(to_send(peers[k], me_l), landed(peer, me_l), rh_s.at[k], rh_r.at[k], peers[k], me_l)

    def pass_on(k, q, where, send_sem, recv_sem):
        part = landed(peers[k], q)
        return remote(part, part, send_sem.at[k], recv_sem.at[k], me_r, where)

    pl.semaphore_wait(pltpu.get_barrier_semaphore(), 15)
    sum_start((part, zero), 2, *sums)
    for off in range(1, 4):
        r_quarter(off, me_r).start()
    get_l(0).start()

    @pl.loop(0, groups)
    def _(g):
        col = pl.ds(pl.multiple_of(me_r * bl, bl), bl)
        u2[groups + g, bl:bl + block, col] = u2[g, bl:bl + block, col]

    vg[...] = jnp.zeros(vg.shape, F32)
    norm = jnp.sqrt(sum_end(2, *sums)[0] / cfg.elems)
    cf[0] = zero
    cf[1] = 1.0 / norm
    cf[2] = zero
    cf[3] = zero + 1.0
    cf[4] = norm
    sum_sent(2, *sums)
    for off in range(1, 4):
        r_quarter(off, peers[off]).wait_recv()
        pass_on(off, me_l, across, rx_s, rx_r).start()
        pass_on(off, me_l, mate, rm_s, rm_r).start()
    for off in range(1, 4):
        r_quarter(off, me_r).wait_send()
    for h in range(2):
        for off in range(1, 4):
            ag_copy(h, off).start()
    for off in range(1, 4):
        pass_on(off, across, across, rx_s, rx_r).wait_recv()
        pass_on(off, across, mate, rn_s, rn_r).start()
    for off in range(1, 4):
        pass_on(off, mate, mate, rm_s, rm_r).wait_recv()
        pass_on(off, diag, mate, rn_s, rn_r).wait_recv()
    lanes = nb // 2
    lowb = lax.broadcasted_iota(jnp.int32, (8, lanes), 0) < 4

    @pl.loop(0, groups)
    def _(g):
        for e in range(2):
            raw = u2[groups + g, bl:bl + block, e * lanes:(e + 1) * lanes].reshape(W, 16, lanes)
            for b8 in range(2):
                cols = raw[:, 8 * b8:8 * b8 + 8]
                one = jnp.transpose(cols[0:8], (1, 0, 2))
                two = jnp.transpose(cols[8:16], (1, 0, 2))
                tail = jnp.transpose(jnp.concatenate([cols[16:20], cols[16:20]], axis=0), (1, 0, 2))
                for quad in range(2):
                    b0 = 4 * quad
                    parts = []
                    for b in range(b0, b0 + 4):
                        parts += [one[b], two[b]]
                    parts += [jnp.where(lowb, tail[b0], tail[b0 + 1]), jnp.where(lowb, tail[b0 + 2], tail[b0 + 3])]
                    at = pl.ds(pl.multiple_of(g * block + 160 * b8 + 80 * quad, 16), 80)
                    for k, v in enumerate(split3(jnp.concatenate(parts, axis=0))):
                        rts[k, at, e * lanes:(e + 1) * lanes] = v

    for off in range(1, 4):
        pass_on(off, me_l, across, rx_s, rx_r).wait_send()
        pass_on(off, me_l, mate, rm_s, rm_r).wait_send()
        pass_on(off, across, mate, rn_s, rn_r).wait_send()

    def norm_start():
        part = zero
        for h in range(2):
            for s in range(S):
                w = (qg[h, s, own, :] - coef(0, (bl, lt)) * vg[h, s, own, :]) * coef(1, (bl, lt))
                part = part + fold(w * w)
        sum_start((part, zero), 1, *sums)

    def norm_end(j):
        gamma = jnp.sqrt(sum_end(1, *sums)[0] / cfg.elems)
        beta = gamma * cf[4]
        out_s[STEPS + j] = beta
        cf[2] = beta * cf[3]
        cf[3] = 1.0 / gamma
        sum_sent(1, *sums)

    @pl.loop(0, STEPS)
    def _(j):
        update(0, j)
        group(0, ub0, ub1, do_w=False)

        @pl.when(j > 0)
        def _():
            norm_end(j - 1)

        group(1, ub1, ub0)

        @pl.loop(1, groups)
        def _(p):
            @pl.when(p == groups // 2)
            def _():
                update(1, j)

            group(2 * p, ub0, ub1)
            group(2 * p + 1, ub1, ub0)

        group(2 * groups, ub0, ub1, do_r=False)
        al[...] = jnp.zeros((16, 128), F32)
        acc[...] = jnp.zeros((rows, lt), F32)

        @pl.loop(0, 8 * trips)
        def _(n):
            l_trip(n)

            @pl.when(lax.rem(n, trips) == trips - 1)
            def _():
                send_on(n // trips, j)
                acc[...] = jnp.zeros((rows, lt), F32)

        sum_start((al[0:8], al[8:16]), 0, *sums)
        dot, square = sum_end(0, *sums)
        alpha = cf[3] * (dot / cfg.elems)
        size = jnp.sqrt(square / cfg.elems)
        size = jnp.where(size > 0.0, size, 1.0)
        out_s[j] = alpha
        cf[0] = alpha * cf[3]
        cf[1] = 1.0 / size
        cf[4] = size
        norm_start()

        @pl.when(j < STEPS - 1)
        def _():
            ag_start(1)

        sum_sent(0, *sums)

    norm_end(STEPS - 1)
    get_l(0).wait()
    for h in range(2):
        for s in range(S):
            v = (qg[h, s, own, :] - coef(0, (bl, lt)) * vg[h, s, own, :]) * coef(1, (bl, lt))
            qg[h, s, own, :] = v * coef(3, (bl, lt))
    result = pltpu.make_async_copy(qg.at[:, :, own, :], out_v, qsem)
    result.start()
    result.wait()


def steps(cfg, l3, rb3, psi, wl):
    lt, bl, nb, rows = cfg.lt, cfg.bl, cfg.nb, cfg.rows
    hbm = pl.BlockSpec(memory_space=pl.ANY)
    vm = pl.BlockSpec(memory_space=pltpu.VMEM)
    dma = pltpu.SemaphoreType.DMA
    block = (cfg.nl, rows, lt // cfg.nl)
    scratch = [
        pltpu.VMEM((W, rows, cfg.a), F32),
        pltpu.VMEM((3, W * bl, nb), BF),
        pltpu.VMEM((3, S, nb, lt), BF),
        pltpu.VMEM((2, S, nb, lt), F32),
        pltpu.VMEM((2, S, nb, lt), F32),
        pltpu.VMEM((2, CH, cfg.a, lt), F32),
        pltpu.VMEM((3, *block), F32),
        pltpu.VMEM(block, F32),
        pltpu.VMEM(block, F32),
        pltpu.VMEM((2, *block), F32),
        pltpu.VMEM((4, 4 * W, lt), F32),
        pltpu.VMEM((2, S, bl, lt), F32),
        pltpu.VMEM((rows, lt), F32),
        pltpu.VMEM((5, 8, 128), F32),
        pltpu.VMEM((16, 128), F32),
        pltpu.VMEM((3, 16, 128), F32),
        pltpu.VMEM((3, 16, 16, 128), F32),
        dma((2,)), dma((4,)), dma, dma((3, 16)), dma((3, 16)), dma((3,)), dma((4,)), dma((2, 4)), dma((2, 4)),
        dma((4,)), dma((4,)), dma((4,)), dma((4,)), dma((4,)), dma((4,)), dma((4,)), dma((4,)),
        pltpu.SemaphoreType.REGULAR((2,)),
    ]
    return pl.pallas_call(
        functools.partial(kernel, cfg),
        out_shape=(
            jax.ShapeDtypeStruct((2, S, bl, lt), F32),
            jax.ShapeDtypeStruct((2 * STEPS, 8, 128), F32),
        ),
        in_specs=[hbm, hbm, hbm, vm],
        out_specs=(hbm, vm),
        scratch_shapes=scratch,
        compiler_params=pltpu.CompilerParams(collective_id=0, has_side_effects=True, vmem_limit_bytes=VM_LIMIT),
    )(l3, rb3, psi, wl)


def mpo_rows(mpo_two):
    w = mpo_two.reshape(W, W, S, S).transpose(0, 3, 2, 1)
    w = jnp.concatenate([w[..., :16].reshape(W * S, 64), w[..., 16:].reshape(W * S, 16)], axis=1)
    one = lax.reduce_precision(w, 8, 7)
    two = lax.reduce_precision(w - one, 8, 7)
    three = w - one - two
    none = jnp.zeros_like(w)
    left = jnp.concatenate([
        jnp.concatenate([one, one, one], 1),
        jnp.concatenate([two, two, none], 1),
        jnp.concatenate([three, none, none], 1)], 0)
    return jnp.pad(left, ((0, 0), (0, 16))).astype(BF)


def build(mesh, cfg):
    def lanczos(psi_block, left_env, right_env, mpo_two):
        lt, a, bl = cfg.lt, cfg.a, cfg.bl
        l3 = jnp.transpose(left_env, (1, 0, 2))
        rb3 = jnp.transpose(right_env, (1, 0, 2))
        psi = psi_block.reshape(4, a, bl)
        wl = mpo_rows(mpo_two)
        vec, scal = steps(cfg, l3, rb3, psi, wl)
        vec = vec.transpose(0, 3, 1, 2).reshape(psi_block.shape)
        return scal[:STEPS, 0, 0], scal[STEPS:, 0, 0], vec

    return jax.shard_map(
        lanczos,
        mesh=mesh,
        in_specs=(P('left', None, None, 'right'), P('left', None, None), P('right', None, None), P()),
        out_specs=(P(), P(), P('left', None, None, 'right')),
        check_vma=False,
    )


def solution(mesh):
    return build(mesh, Cfg())
```

```python
import functools

import jax
import jax.numpy as jnp
from jax import lax
from jax.experimental import pallas as pl
from jax.experimental.pallas import tpu as pltpu
from jax.sharding import PartitionSpec as P

STEPS = 4
W = 20
S = 4
BF = jnp.bfloat16
F32 = jnp.float32
VM_LIMIT = 67043328


class Cfg:
    def __init__(self, lt=256, bl=128):
        self.lt = lt
        self.a = 2 * lt
        self.bl = bl
        self.nb = 4 * bl
        self.kb = self.nb // 2
        self.groups = bl // 16
        self.rows = 4 * bl
        self.nl = max(lt // 128, 1)
        self.elems = float(4 * self.a * S * self.nb)


def split3(x):
    one = x.astype(BF)
    rest = x - one.astype(F32)
    two = rest.astype(BF)
    return one, two, (rest - two.astype(F32)).astype(BF)


def remote(src, dst, send_sem, recv_sem, right, left):
    return pltpu.make_async_remote_copy(
        src_ref=src, dst_ref=dst, send_sem=send_sem, recv_sem=recv_sem,
        device_id={'right': right, 'left': left}, device_id_type=pl.DeviceIdType.MESH)


def enter(me):
    barrier = pltpu.get_barrier_semaphore()

    @pl.loop(1, 16)
    def _(off):
        peer = lax.rem(me + off, 16)
        pl.semaphore_signal(barrier, 1, device_id={'right': peer // 4, 'left': lax.rem(peer, 4)},
                            device_id_type=pl.DeviceIdType.MESH)


def sum_copy(k, me, peer, slot, out_ref, in_ref, send_sem, recv_sem):
    return remote(out_ref.at[k], in_ref.at[k, slot], send_sem.at[k, peer], recv_sem.at[k, slot], peer // 4, lax.rem(peer, 4))


def sum_start(parts, k, me, *refs):
    out_ref, in_ref = refs[:2]
    for i, part in enumerate(parts):
        out_ref[k, 8 * i:8 * i + 8] = part
        in_ref[k, me, 8 * i:8 * i + 8] = part

    @pl.loop(1, 16)
    def _(off):
        sum_copy(k, me, lax.rem(me + off, 16), me, *refs).start()


def sum_end(k, me, *refs):
    @pl.loop(1, 16)
    def _(off):
        peer = lax.rem(me + off, 16)
        sum_copy(k, me, peer, peer, *refs).wait_recv()

    total = refs[1][k, 0]
    for i in range(1, 16):
        total = total + refs[1][k, i]

    total = jnp.sum(total, axis=1, keepdims=True)
    return [jnp.broadcast_to(jnp.sum(total[8 * i:8 * i + 8], axis=0, keepdims=True), (8, 128)) for i in range(2)]


def sum_sent(k, me, *refs):
    @pl.loop(1, 16)
    def _(off):
        sum_copy(k, me, lax.rem(me + off, 16), me, *refs).wait_send()


def fold(x):
    r, c = x.shape
    if c % 128 == 0:
        x = jnp.sum(x.reshape(r // 8, 8, c), axis=0)
        acc = x[:, :128]
        for i in range(1, c // 128):
            acc = acc + x[:, i * 128:(i + 1) * 128]
        return acc
    return jnp.full((8, 128), jnp.sum(x) / 1024.0, F32)


CH = 10


def kernel(cfg, l3, rb3, psi, wl, out_v, out_s,
           u2, rts, vgs, vg, qg, lb, sb, rb0, yb, xs, ob, vp, acc, cf, al, ars, arr,
           lsem, psem, qsem, ar_s, ar_r, rs_s, rs_r, ag_s, ag_r, rh_s, rh_r, rx_s, rx_r, rm_s, rm_r, rn_s, rn_r, credit):
    lt, bl, nb, kb, rows, groups = cfg.lt, cfg.bl, cfg.nb, cfg.kb, cfg.rows, cfg.groups
    nl, lw = cfg.nl, cfg.lt // cfg.nl
    me_r = lax.axis_index('right')
    me_l = lax.axis_index('left')
    me = me_r * 4 + me_l
    core = lax.rem(me_l, 2)
    chip = me_l // 2
    mate = chip * 2 + 1 - core
    across = (1 - chip) * 2 + core
    diag = (1 - chip) * 2 + 1 - core
    peers = (me_r, me_r + 1 - 2 * lax.rem(me_r, 2), lax.rem(me_r + 2, 4), 3 - me_r)
    own = pl.ds(pl.multiple_of(me_r * bl, bl), bl)
    ub0 = lb.at[1, 0:S, 0:16 * W]
    ub1 = lb.at[1, S:2 * S, 0:16 * W]
    sums = (me, ars, arr, ar_s, ar_r)
    zero = jnp.zeros((8, 128), F32)
    trips = W // CH
    low = lax.broadcasted_iota(jnp.int32, (8, lt), 0) < 4

    def get_l(n):
        tile = lax.rem(n // trips, 8)
        h, who = tile // 4, lax.rem(tile, 4)
        to = lax.rem(chip + 1 - who // 2, 2) * 2 + lax.rem(core + 1 - lax.rem(who, 2), 2)
        col = pl.ds(pl.multiple_of((2 * to + h) * lt, lt), lt)
        slot = lax.rem(n, 2)
        return pltpu.make_async_copy(l3.at[pl.ds(lax.rem(n, trips) * CH, CH), :, col], lb.at[slot], lsem.at[slot])

    def ag_copy(h, k):
        return remote(qg.at[h, :, own, :], qg.at[h, :, own, :], ag_s.at[h, k], ag_r.at[h, k], peers[k], me_l)

    def ag_from(h, k):
        there = qg.at[h, :, pl.ds(pl.multiple_of(peers[k] * bl, bl), bl), :]
        return remote(there, there, ag_s.at[h, k], ag_r.at[h, k], peers[k], me_l)

    def coef(i, shape):
        one = cf[i, 0:1, 0:1]
        return jnp.broadcast_to(one, shape)

    def update(h, j):
        for off in range(1, 4):
            ag_from(h, off).wait_recv()
            ag_copy(h, off).wait_send()

        for s in range(S):
            vp[h, s] = vg[h, s, own, :]
        chunk = min(256, nb)

        @pl.loop(0, S * (nb // chunk))
        def _(i):
            s = i // (nb // chunk)
            at = pl.ds(pl.multiple_of(lax.rem(i, nb // chunk) * chunk, chunk), chunk)
            new = (qg[h, s, at, :] - coef(0, (chunk, lt)) * vg[h, s, at, :]) * coef(1, (chunk, lt))
            vg[h, s, at, :] = new
            for k, v in enumerate(split3(new)):
                vgs[k, s, at, :] = v

        @pl.when(j < STEPS - 1)
        def _():
            for off in range(1, 4):
                pl.semaphore_signal(credit.at[h], 1, device_id={'right': peers[off], 'left': me_l},
                                    device_id_type=pl.DeviceIdType.MESH)

    def w_tile(ub, quad, i):
        base = 80 * quad
        pair = base + 64 + 8 * (i // 2)
        parts = [ub[s, base + 16 * i:base + 16 * i + 16, :] for s in range(S)]
        for s in (0, 2):
            one, two = ub[s, pair:pair + 8, :], ub[s + 1, pair:pair + 8, :]
            if i % 2 == 0:
                parts.append(jnp.where(low, one, pltpu.roll(two, 4, 0)))
            else:
                parts.append(jnp.where(low, pltpu.roll(one, 4, 0), two))
        x = jnp.concatenate(parts, axis=0) * coef(3, (4 * W, lt))
        return jnp.concatenate([*split3(x), jnp.zeros((16, lt), BF)], axis=0)

    def w_finish(quad, g, h):
        even, odd = [], []
        for i in range(W // 2):
            v = [ob[b, 8 * i:8 * i + 8, :] for b in range(4)]
            for dst, b0 in ((even, 0), (even, 2)):
                dst.append(jnp.where(low, v[b0], pltpu.roll(v[b0 + 1], 4, 0)))
            for dst, b0 in ((odd, 0), (odd, 2)):
                dst.append(jnp.where(low, pltpu.roll(v[b0], 4, 0), v[b0 + 1]))
        at = pl.ds(pl.multiple_of(g * 64 + 16 * quad, 16), 16)
        col = pl.ds(pl.multiple_of(h * lt, lt), lt)
        for first, lst in ((0, even), (1, odd)):
            for i in range(W // 2):
                u2[2 * i + first, at, col] = jnp.concatenate(lst[2 * i:2 * i + 2], axis=0)

    def group(it, ub_new, ub_old, do_r=True, do_w=True):
        before = lax.rem(it + 2 * groups - 1, 2 * groups)
        gw, hw = lax.rem(before, groups), before // groups
        at = pl.ds(pl.multiple_of(lax.rem(it, groups) * (16 * W), 16 * W), 16 * W)
        for s in range(S):
            if do_r:
                total = None
                for k in range(3):
                    for i in range(3 - k):
                        term = jnp.dot(rts[i, at, :], vgs[k, s], preferred_element_type=F32)
                        total = term if total is None else total + term
                ub_new[s] = total
            if not do_w:
                continue
            for i in range(4):
                y = jnp.dot(wl[...], w_tile(ub_old, s, i), preferred_element_type=F32)
                ob[i] = (y[:4 * W] + y[4 * W:8 * W]) + y[8 * W:]
            w_finish(s, gw, hw)

    def l_trip(n):
        get_l(n).wait()
        get_l(n + 1).start()
        slot, l0 = lax.rem(n, 2), lax.rem(n, trips) * CH
        total = None
        for m in range(CH):
            left, right = split3(u2[l0 + m]), split3(lb[slot, m])
            for k in range(3):
                for i in range(3 - k):
                    term = jnp.dot(left[i], right[k], preferred_element_type=F32)
                    total = term if total is None else total + term
        acc[...] += total

    def rs_copy(k, h):
        dst = (rb0, xs.at[h], yb)[k]
        i = 1 + h if k == 1 else (0 if k == 0 else 3)
        return remote(sb.at[k], dst, rs_s.at[k], rs_r.at[i], me_r, across if k == 1 else mate)

    def part_of(i):
        return acc[:, i * lw:(i + 1) * lw]

    def send_on(n, j):
        h, who = n // 4, lax.rem(n, 4)

        @pl.when(who == 0)
        def _():
            for i in range(nl):
                sb[0, i] = part_of(i)
            rs_copy(0, h).start()

        @pl.when(who == 1)
        def _():
            rs_copy(0, h).wait_recv()
            for i in range(nl):
                sb[1, i] = part_of(i) + rb0[i]
            rs_copy(1, h).start()

        @pl.when(who == 2)
        def _():
            rs_copy(0, h).wait_send()
            for i in range(nl):
                sb[2, i] = part_of(i)
            rs_copy(2, h).start()

        @pl.when(who == 3)
        def _():
            finish(h, j)

    def finish(h, j):
        rs_copy(2, h).wait_recv()
        rs_copy(1, h).wait_recv()
        for i in range(nl):
            yb[i] = (part_of(i) + yb[i]) + xs[h, i]
        rs_copy(1, h).wait_send()
        rs_copy(2, h).wait_send()
        for t in range(S):
            w = jnp.concatenate([yb[i, pl.ds(t, bl, stride=4), :] for i in range(nl)], axis=1)
            q = w - coef(2, (bl, lt)) * vp[h, t]
            al[0:8] += fold(w * vg[h, t, own, :])
            al[8:16] += fold(q * q)
            qg[h, t, own, :] = q

        @pl.when((j < STEPS - 1) & (h == 0))
        def _():
            ag_start(0)

    def ag_start(h):
        pl.semaphore_wait(credit.at[h], 3)
        for off in range(1, 4):
            ag_copy(h, off).start()

    def get_psi(i):
        return pltpu.make_async_copy(psi.at[i], sb.at[i // 2, i % 2], psem.at[i])

    load_r = pltpu.make_async_copy(rb3, u2.at[:, 0:bl, :], qsem)
    load_r.start()
    for i in range(4):
        get_psi(i).start()
    enter(me)
    part = zero
    for i in range(4):
        get_psi(i).wait()
        for s in range(S):
            x = sb[i // 2, i % 2, pl.ds(s, bl, stride=S), :]
            part = part + fold(x * x)
            qg[i // 2, s, own, (i % 2) * lw:(i % 2 + 1) * lw] = x.T
    load_r.wait()
    block = 16 * W

    @pl.loop(0, W)
    def _(r):
        at = pl.ds(pl.multiple_of(bl + r * 16, 16), 16)
        turned = [u2[r, 0:bl, p * bl:(p + 1) * bl].T for p in range(4)]
        for p, x in enumerate(turned):
            for g in range(groups):
                u2[g, at, p * bl:(p + 1) * bl] = x[16 * g:16 * g + 16]

    def to_send(peer, q):
        return u2.at[0:groups, pl.ds(pl.multiple_of(bl + q * (block // 4), 8), block // 4),
                     pl.ds(pl.multiple_of(peer * bl, bl), bl)]

    def landed(peer, q):
        return u2.at[groups:2 * groups, pl.ds(pl.multiple_of(bl + q * (block // 4), 8), block // 4),
                     pl.ds(pl.multiple_of(peer * bl, bl), bl)]

    def r_quarter(k, peer):
        return remote(to_send(peers[k], me_l), landed(peer, me_l), rh_s.at[k], rh_r.at[k], peers[k], me_l)

    def pass_on(k, q, where, send_sem, recv_sem):
        part = landed(peers[k], q)
        return remote(part, part, send_sem.at[k], recv_sem.at[k], me_r, where)

    pl.semaphore_wait(pltpu.get_barrier_semaphore(), 15)
    sum_start((part, zero), 2, *sums)
    for off in range(1, 4):
        r_quarter(off, me_r).start()
    get_l(0).start()

    @pl.loop(0, groups)
    def _(g):
        col = pl.ds(pl.multiple_of(me_r * bl, bl), bl)
        u2[groups + g, bl:bl + block, col] = u2[g, bl:bl + block, col]

    vg[...] = jnp.zeros(vg.shape, F32)
    norm = jnp.sqrt(sum_end(2, *sums)[0] / cfg.elems)
    cf[0] = zero
    cf[1] = 1.0 / norm
    cf[2] = zero
    cf[3] = zero + 1.0
    cf[4] = norm
    sum_sent(2, *sums)
    for off in range(1, 4):
        r_quarter(off, peers[off]).wait_recv()
        pass_on(off, me_l, across, rx_s, rx_r).start()
        pass_on(off, me_l, mate, rm_s, rm_r).start()
        if off > 1:
            for k in range(1, 4):
                ag_copy(off - 2, k).start()
    for off in range(1, 4):
        pass_on(off, across, across, rx_s, rx_r).wait_recv()
        pass_on(off, across, mate, rn_s, rn_r).start()
    for off in range(1, 4):
        pass_on(off, mate, mate, rm_s, rm_r).wait_recv()
        pass_on(off, diag, mate, rn_s, rn_r).wait_recv()
    lanes = nb // 2
    lowb = lax.broadcasted_iota(jnp.int32, (8, lanes), 0) < 4

    @pl.loop(0, groups)
    def _(g):
        for e in range(2):
            raw = u2[groups + g, bl:bl + block, e * lanes:(e + 1) * lanes].reshape(W, 16, lanes)
            for b8 in range(2):
                cols = raw[:, 8 * b8:8 * b8 + 8]
                one = jnp.transpose(cols[0:8], (1, 0, 2))
                two = jnp.transpose(cols[8:16], (1, 0, 2))
                tail = jnp.transpose(jnp.concatenate([cols[16:20], cols[16:20]], axis=0), (1, 0, 2))
                for quad in range(2):
                    b0 = 4 * quad
                    parts = []
                    for b in range(b0, b0 + 4):
                        parts += [one[b], two[b]]
                    parts += [jnp.where(lowb, tail[b0], tail[b0 + 1]), jnp.where(lowb, tail[b0 + 2], tail[b0 + 3])]
                    at = pl.ds(pl.multiple_of(g * block + 160 * b8 + 80 * quad, 16), 80)
                    for k, v in enumerate(split3(jnp.concatenate(parts, axis=0))):
                        rts[k, at, e * lanes:(e + 1) * lanes] = v

    for off in range(1, 4):
        r_quarter(off, me_r).wait_send()
        pass_on(off, me_l, across, rx_s, rx_r).wait_send()
        pass_on(off, me_l, mate, rm_s, rm_r).wait_send()
        pass_on(off, across, mate, rn_s, rn_r).wait_send()

    def norm_start():
        part = zero
        for h in range(2):
            for s in range(S):
                w = (qg[h, s, own, :] - coef(0, (bl, lt)) * vg[h, s, own, :]) * coef(1, (bl, lt))
                part = part + fold(w * w)
        sum_start((part, zero), 1, *sums)

    def norm_end(j):
        gamma = jnp.sqrt(sum_end(1, *sums)[0] / cfg.elems)
        beta = gamma * cf[4]
        out_s[STEPS + j] = beta
        cf[2] = beta * cf[3]
        cf[3] = 1.0 / gamma
        sum_sent(1, *sums)

    @pl.loop(0, STEPS)
    def _(j):
        update(0, j)
        group(0, ub0, ub1, do_w=False)

        @pl.when(j > 0)
        def _():
            norm_end(j - 1)

        group(1, ub1, ub0)

        @pl.loop(1, groups)
        def _(p):
            @pl.when(p == groups // 2)
            def _():
                update(1, j)

            group(2 * p, ub0, ub1)
            group(2 * p + 1, ub1, ub0)

        group(2 * groups, ub0, ub1, do_r=False)
        al[...] = jnp.zeros((16, 128), F32)
        acc[...] = jnp.zeros((rows, lt), F32)

        @pl.loop(0, 8 * trips)
        def _(n):
            l_trip(n)

            @pl.when(lax.rem(n, trips) == trips - 1)
            def _():
                send_on(n // trips, j)
                acc[...] = jnp.zeros((rows, lt), F32)

        sum_start((al[0:8], al[8:16]), 0, *sums)
        dot, square = sum_end(0, *sums)
        alpha = cf[3] * (dot / cfg.elems)
        size = jnp.sqrt(square / cfg.elems)
        size = jnp.where(size > 0.0, size, 1.0)
        out_s[j] = alpha
        cf[0] = alpha * cf[3]
        cf[1] = 1.0 / size
        cf[4] = size
        norm_start()

        @pl.when(j < STEPS - 1)
        def _():
            ag_start(1)

        sum_sent(0, *sums)

    norm_end(STEPS - 1)
    get_l(0).wait()
    for h in range(2):
        for s in range(S):
            v = (qg[h, s, own, :] - coef(0, (bl, lt)) * vg[h, s, own, :]) * coef(1, (bl, lt))
            qg[h, s, own, :] = v * coef(3, (bl, lt))
    result = pltpu.make_async_copy(qg.at[:, :, own, :], out_v, qsem)
    result.start()
    result.wait()


def steps(cfg, l3, rb3, psi, wl):
    lt, bl, nb, rows = cfg.lt, cfg.bl, cfg.nb, cfg.rows
    hbm = pl.BlockSpec(memory_space=pl.ANY)
    vm = pl.BlockSpec(memory_space=pltpu.VMEM)
    dma = pltpu.SemaphoreType.DMA
    block = (cfg.nl, rows, lt // cfg.nl)
    scratch = [
        pltpu.VMEM((W, rows, cfg.a), F32),
        pltpu.VMEM((3, W * bl, nb), BF),
        pltpu.VMEM((3, S, nb, lt), BF),
        pltpu.VMEM((2, S, nb, lt), F32),
        pltpu.VMEM((2, S, nb, lt), F32),
        pltpu.VMEM((2, CH, cfg.a, lt), F32),
        pltpu.VMEM((3, *block), F32),
        pltpu.VMEM(block, F32),
        pltpu.VMEM(block, F32),
        pltpu.VMEM((2, *block), F32),
        pltpu.VMEM((4, 4 * W, lt), F32),
        pltpu.VMEM((2, S, bl, lt), F32),
        pltpu.VMEM((rows, lt), F32),
        pltpu.VMEM((5, 8, 128), F32),
        pltpu.VMEM((16, 128), F32),
        pltpu.VMEM((3, 16, 128), F32),
        pltpu.VMEM((3, 16, 16, 128), F32),
        dma((2,)), dma((4,)), dma, dma((3, 16)), dma((3, 16)), dma((3,)), dma((4,)), dma((2, 4)), dma((2, 4)),
        dma((4,)), dma((4,)), dma((4,)), dma((4,)), dma((4,)), dma((4,)), dma((4,)), dma((4,)),
        pltpu.SemaphoreType.REGULAR((2,)),
    ]
    return pl.pallas_call(
        functools.partial(kernel, cfg),
        out_shape=(
            jax.ShapeDtypeStruct((2, S, bl, lt), F32),
            jax.ShapeDtypeStruct((2 * STEPS, 8, 128), F32),
        ),
        in_specs=[hbm, hbm, hbm, vm],
        out_specs=(hbm, vm),
        scratch_shapes=scratch,
        compiler_params=pltpu.CompilerParams(collective_id=0, has_side_effects=True, vmem_limit_bytes=VM_LIMIT),
    )(l3, rb3, psi, wl)


def mpo_rows(mpo_two):
    w = mpo_two.reshape(W, W, S, S).transpose(0, 3, 2, 1)
    w = jnp.concatenate([w[..., :16].reshape(W * S, 64), w[..., 16:].reshape(W * S, 16)], axis=1)
    one = lax.reduce_precision(w, 8, 7)
    two = lax.reduce_precision(w - one, 8, 7)
    three = w - one - two
    none = jnp.zeros_like(w)
    left = jnp.concatenate([
        jnp.concatenate([one, one, one], 1),
        jnp.concatenate([two, two, none], 1),
        jnp.concatenate([three, none, none], 1)], 0)
    return jnp.pad(left, ((0, 0), (0, 16))).astype(BF)


def build(mesh, cfg):
    def lanczos(psi_block, left_env, right_env, mpo_two):
        lt, a, bl = cfg.lt, cfg.a, cfg.bl
        l3 = jnp.transpose(left_env, (1, 0, 2))
        rb3 = jnp.transpose(right_env, (1, 0, 2))
        psi = psi_block.reshape(4, a, bl)
        wl = mpo_rows(mpo_two)
        vec, scal = steps(cfg, l3, rb3, psi, wl)
        vec = vec.transpose(0, 3, 1, 2).reshape(psi_block.shape)
        return scal[:STEPS, 0, 0], scal[STEPS:, 0, 0], vec

    return jax.shard_map(
        lanczos,
        mesh=mesh,
        in_specs=(P('left', None, None, 'right'), P('left', None, None), P('right', None, None), P()),
        out_specs=(P(), P(), P('left', None, None, 'right')),
        check_vma=False,
    )


def solution(mesh):
    return build(mesh, Cfg())
```

```python
import functools

import jax
import jax.numpy as jnp
from jax import lax
from jax.experimental import pallas as pl
from jax.experimental.pallas import tpu as pltpu
from jax.sharding import PartitionSpec as P

STEPS = 4
W = 20
S = 4
BF = jnp.bfloat16
F32 = jnp.float32
VM_LIMIT = 67043328


class Cfg:
    def __init__(self, lt=256, bl=128):
        self.lt = lt
        self.a = 2 * lt
        self.bl = bl
        self.nb = 4 * bl
        self.kb = self.nb // 2
        self.groups = bl // 16
        self.rows = 4 * bl
        self.nl = max(lt // 128, 1)
        self.elems = float(4 * self.a * S * self.nb)


def split3(x):
    one = x.astype(BF)
    rest = x - one.astype(F32)
    two = rest.astype(BF)
    return one, two, (rest - two.astype(F32)).astype(BF)


def remote(src, dst, send_sem, recv_sem, right, left):
    return pltpu.make_async_remote_copy(
        src_ref=src, dst_ref=dst, send_sem=send_sem, recv_sem=recv_sem,
        device_id={'right': right, 'left': left}, device_id_type=pl.DeviceIdType.MESH)


def enter(me):
    barrier = pltpu.get_barrier_semaphore()

    @pl.loop(1, 16)
    def _(off):
        peer = lax.rem(me + off, 16)
        pl.semaphore_signal(barrier, 1, device_id={'right': peer // 4, 'left': lax.rem(peer, 4)},
                            device_id_type=pl.DeviceIdType.MESH)


def sum_copy(k, me, peer, slot, out_ref, in_ref, send_sem, recv_sem):
    return remote(out_ref.at[k], in_ref.at[k, slot], send_sem.at[k, peer], recv_sem.at[k, slot], peer // 4, lax.rem(peer, 4))


def sum_start(parts, k, me, *refs):
    out_ref, in_ref = refs[:2]
    for i, part in enumerate(parts):
        out_ref[k, 8 * i:8 * i + 8] = part
        in_ref[k, me, 8 * i:8 * i + 8] = part

    for off in range(1, 16):
        sum_copy(k, me, lax.rem(me + off, 16), me, *refs).start()


def sum_end(k, me, *refs):
    @pl.loop(1, 16)
    def _(off):
        peer = lax.rem(me + off, 16)
        sum_copy(k, me, peer, peer, *refs).wait_recv()

    total = refs[1][k, 0]
    for i in range(1, 16):
        total = total + refs[1][k, i]

    total = jnp.sum(total, axis=1, keepdims=True)
    return [jnp.broadcast_to(jnp.sum(total[8 * i:8 * i + 8], axis=0, keepdims=True), (8, 128)) for i in range(2)]


def sum_sent(k, me, *refs):
    @pl.loop(1, 16)
    def _(off):
        sum_copy(k, me, lax.rem(me + off, 16), me, *refs).wait_send()


def fold(x):
    r, c = x.shape
    if c % 128 == 0:
        x = jnp.sum(x.reshape(r // 8, 8, c), axis=0)
        acc = x[:, :128]
        for i in range(1, c // 128):
            acc = acc + x[:, i * 128:(i + 1) * 128]
        return acc
    return jnp.full((8, 128), jnp.sum(x) / 1024.0, F32)


CH = 10


def kernel(cfg, l3, rb3, psi, wl, out_v, out_s,
           u2, rts, vgs, vg, qg, lb, sb, rb0, yb, xs, ob, vp, acc, cf, al, ars, arr,
           lsem, psem, qsem, ar_s, ar_r, rs_s, rs_r, ag_s, ag_r, rh_s, rh_r, rx_s, rx_r, rm_s, rm_r, rn_s, rn_r, credit):
    lt, bl, nb, kb, rows, groups = cfg.lt, cfg.bl, cfg.nb, cfg.kb, cfg.rows, cfg.groups
    nl, lw = cfg.nl, cfg.lt // cfg.nl
    me_r = lax.axis_index('right')
    me_l = lax.axis_index('left')
    me = me_r * 4 + me_l
    core = lax.rem(me_l, 2)
    chip = me_l // 2
    mate = chip * 2 + 1 - core
    across = (1 - chip) * 2 + core
    diag = (1 - chip) * 2 + 1 - core
    peers = (me_r, me_r + 1 - 2 * lax.rem(me_r, 2), lax.rem(me_r + 2, 4), 3 - me_r)
    own = pl.ds(pl.multiple_of(me_r * bl, bl), bl)
    ub0 = lb.at[1, 0:S, 0:16 * W]
    ub1 = lb.at[1, S:2 * S, 0:16 * W]
    sums = (me, ars, arr, ar_s, ar_r)
    zero = jnp.zeros((8, 128), F32)
    trips = W // CH
    low = lax.broadcasted_iota(jnp.int32, (8, lt), 0) < 4

    def get_l(n):
        tile = lax.rem(n // trips, 8)
        h, who = tile // 4, lax.rem(tile, 4)
        to = lax.rem(chip + 1 - who // 2, 2) * 2 + lax.rem(core + 1 - lax.rem(who, 2), 2)
        col = pl.ds(pl.multiple_of((2 * to + h) * lt, lt), lt)
        slot = lax.rem(n, 2)
        return pltpu.make_async_copy(l3.at[pl.ds(lax.rem(n, trips) * CH, CH), :, col], lb.at[slot], lsem.at[slot])

    def ag_copy(h, k):
        return remote(qg.at[h, :, own, :], qg.at[h, :, own, :], ag_s.at[h, k], ag_r.at[h, k], peers[k], me_l)

    def ag_from(h, k):
        there = qg.at[h, :, pl.ds(pl.multiple_of(peers[k] * bl, bl), bl), :]
        return remote(there, there, ag_s.at[h, k], ag_r.at[h, k], peers[k], me_l)

    def coef(i, shape):
        one = cf[i, 0:1, 0:1]
        return jnp.broadcast_to(one, shape)

    def update(h, j):
        for off in range(1, 4):
            ag_from(h, off).wait_recv()
            ag_copy(h, off).wait_send()

        for s in range(S):
            vp[h, s] = vg[h, s, own, :]
        chunk = min(256, nb)

        def rows_of(i):
            return i // (nb // chunk), pl.ds(pl.multiple_of(lax.rem(i, nb // chunk) * chunk, chunk), chunk)

        @pl.loop(0, S * (nb // chunk))
        def _(i):
            s, at = rows_of(i)
            vg[h, s, at, :] = (qg[h, s, at, :] - coef(0, (chunk, lt)) * vg[h, s, at, :]) * coef(1, (chunk, lt))

        @pl.loop(0, S * (nb // chunk))
        def _(i):
            s, at = rows_of(i)
            for k, v in enumerate(split3(vg[h, s, at, :])):
                vgs[k, s, at, :] = v

        @pl.when(j < STEPS - 1)
        def _():
            for off in range(1, 4):
                pl.semaphore_signal(credit.at[h], 1, device_id={'right': peers[off], 'left': me_l},
                                    device_id_type=pl.DeviceIdType.MESH)

    def w_tile(ub, quad, i):
        base = 80 * quad
        pair = base + 64 + 8 * (i // 2)
        parts = [ub[s, base + 16 * i:base + 16 * i + 16, :] for s in range(S)]
        for s in (0, 2):
            one, two = ub[s, pair:pair + 8, :], ub[s + 1, pair:pair + 8, :]
            if i % 2 == 0:
                parts.append(jnp.where(low, one, pltpu.roll(two, 4, 0)))
            else:
                parts.append(jnp.where(low, pltpu.roll(one, 4, 0), two))
        x = jnp.concatenate(parts, axis=0) * coef(3, (4 * W, lt))
        return jnp.concatenate([*split3(x), jnp.zeros((16, lt), BF)], axis=0)

    def w_finish(quad, g, h):
        even, odd = [], []
        for i in range(W // 2):
            v = [ob[b, 8 * i:8 * i + 8, :] for b in range(4)]
            for dst, b0 in ((even, 0), (even, 2)):
                dst.append(jnp.where(low, v[b0], pltpu.roll(v[b0 + 1], 4, 0)))
            for dst, b0 in ((odd, 0), (odd, 2)):
                dst.append(jnp.where(low, pltpu.roll(v[b0], 4, 0), v[b0 + 1]))
        at = pl.ds(pl.multiple_of(g * 64 + 16 * quad, 16), 16)
        col = pl.ds(pl.multiple_of(h * lt, lt), lt)
        for first, lst in ((0, even), (1, odd)):
            for i in range(W // 2):
                u2[2 * i + first, at, col] = jnp.concatenate(lst[2 * i:2 * i + 2], axis=0)

    def group(it, ub_new, ub_old, do_r=True, do_w=True):
        before = lax.rem(it + 2 * groups - 1, 2 * groups)
        gw, hw = lax.rem(before, groups), before // groups
        at = pl.ds(pl.multiple_of(lax.rem(it, groups) * (16 * W), 16 * W), 16 * W)
        for s in range(S):
            if do_r:
                total = None
                for k in range(3):
                    for i in range(3 - k):
                        term = jnp.dot(rts[i, at, :], vgs[k, s], preferred_element_type=F32)
                        total = term if total is None else total + term
                ub_new[s] = total
            if not do_w:
                continue
            for i in range(4):
                y = jnp.dot(wl[...], w_tile(ub_old, s, i), preferred_element_type=F32)
                ob[i] = (y[:4 * W] + y[4 * W:8 * W]) + y[8 * W:]
            w_finish(s, gw, hw)

    def l_trip(n):
        get_l(n).wait()
        get_l(n + 1).start()
        slot, l0 = lax.rem(n, 2), lax.rem(n, trips) * CH
        total = None
        for m in range(CH):
            left, right = split3(u2[l0 + m]), split3(lb[slot, m])
            for k in range(3):
                for i in range(3 - k):
                    term = jnp.dot(left[i], right[k], preferred_element_type=F32)
                    total = term if total is None else total + term
        acc[...] += total

    def rs_copy(k, h):
        dst = (rb0, xs.at[h], yb)[k]
        i = 1 + h if k == 1 else (0 if k == 0 else 3)
        return remote(sb.at[k], dst, rs_s.at[k], rs_r.at[i], me_r, across if k == 1 else mate)

    def part_of(i):
        return acc[:, i * lw:(i + 1) * lw]

    def send_on(n, j):
        h, who = n // 4, lax.rem(n, 4)

        @pl.when(who == 0)
        def _():
            for i in range(nl):
                sb[0, i] = part_of(i)
            rs_copy(0, h).start()

        @pl.when(who == 1)
        def _():
            rs_copy(0, h).wait_recv()
            for i in range(nl):
                sb[1, i] = part_of(i) + rb0[i]
            rs_copy(1, h).start()

        @pl.when(who == 2)
        def _():
            rs_copy(0, h).wait_send()
            for i in range(nl):
                sb[2, i] = part_of(i)
            rs_copy(2, h).start()

        @pl.when(who == 3)
        def _():
            finish(h, j)

    def finish(h, j):
        rs_copy(2, h).wait_recv()
        rs_copy(1, h).wait_recv()
        for i in range(nl):
            yb[i] = (part_of(i) + yb[i]) + xs[h, i]
        rs_copy(1, h).wait_send()
        rs_copy(2, h).wait_send()
        for t in range(S):
            w = jnp.concatenate([yb[i, pl.ds(t, bl, stride=4), :] for i in range(nl)], axis=1)
            q = w - coef(2, (bl, lt)) * vp[h, t]
            al[0:8] += fold(w * vg[h, t, own, :])
            al[8:16] += fold(q * q)
            qg[h, t, own, :] = q

        @pl.when((j < STEPS - 1) & (h == 0))
        def _():
            ag_start(0)

    def ag_start(h):
        pl.semaphore_wait(credit.at[h], 3)
        for off in range(1, 4):
            ag_copy(h, off).start()

    def get_psi(i):
        return pltpu.make_async_copy(psi.at[i], sb.at[i // 2, i % 2], psem.at[i])

    load_r = pltpu.make_async_copy(rb3, u2.at[:, 0:bl, :], qsem)
    load_r.start()
    for i in range(4):
        get_psi(i).start()
    enter(me)
    part = zero
    for i in range(4):
        get_psi(i).wait()
        for s in range(S):
            x = sb[i // 2, i % 2, pl.ds(s, bl, stride=S), :]
            part = part + fold(x * x)
            qg[i // 2, s, own, (i % 2) * lw:(i % 2 + 1) * lw] = x.T
    load_r.wait()
    block = 16 * W

    @pl.loop(0, W)
    def _(r):
        at = pl.ds(pl.multiple_of(bl + r * 16, 16), 16)
        turned = [u2[r, 0:bl, p * bl:(p + 1) * bl].T for p in range(4)]
        for p, x in enumerate(turned):
            for g in range(groups):
                u2[g, at, p * bl:(p + 1) * bl] = x[16 * g:16 * g + 16]

    def to_send(peer, q):
        return u2.at[0:groups, pl.ds(pl.multiple_of(bl + q * (block // 4), 8), block // 4),
                     pl.ds(pl.multiple_of(peer * bl, bl), bl)]

    def landed(peer, q):
        return u2.at[groups:2 * groups, pl.ds(pl.multiple_of(bl + q * (block // 4), 8), block // 4),
                     pl.ds(pl.multiple_of(peer * bl, bl), bl)]

    def r_quarter(k, peer):
        return remote(to_send(peers[k], me_l), landed(peer, me_l), rh_s.at[k], rh_r.at[k], peers[k], me_l)

    def pass_on(k, q, where, send_sem, recv_sem):
        part = landed(peers[k], q)
        return remote(part, part, send_sem.at[k], recv_sem.at[k], me_r, where)

    pl.semaphore_wait(pltpu.get_barrier_semaphore(), 15)
    sum_start((part, zero), 2, *sums)
    for off in range(1, 4):
        r_quarter(off, me_r).start()
    get_l(0).start()

    @pl.loop(0, groups)
    def _(g):
        col = pl.ds(pl.multiple_of(me_r * bl, bl), bl)
        u2[groups + g, bl:bl + block, col] = u2[g, bl:bl + block, col]

    vg[...] = jnp.zeros(vg.shape, F32)
    norm = jnp.sqrt(sum_end(2, *sums)[0] / cfg.elems)
    cf[0] = zero
    cf[1] = 1.0 / norm
    cf[2] = zero
    cf[3] = zero + 1.0
    cf[4] = norm
    sum_sent(2, *sums)
    for off in range(1, 4):
        r_quarter(off, peers[off]).wait_recv()
        pass_on(off, me_l, across, rx_s, rx_r).start()
        pass_on(off, me_l, mate, rm_s, rm_r).start()
        if off == 2:
            for k in range(1, 4):
                ag_copy(0, k).start()
    for off in range(1, 4):
        pass_on(off, across, across, rx_s, rx_r).wait_recv()
        pass_on(off, across, mate, rn_s, rn_r).start()
    for off in range(1, 4):
        pass_on(off, mate, mate, rm_s, rm_r).wait_recv()
        pass_on(off, diag, mate, rn_s, rn_r).wait_recv()
    for k in range(1, 4):
        ag_copy(1, k).start()
    lanes = nb // 2
    lowb = lax.broadcasted_iota(jnp.int32, (8, lanes), 0) < 4

    @pl.loop(0, groups)
    def _(g):
        for e in range(2):
            raw = u2[groups + g, bl:bl + block, e * lanes:(e + 1) * lanes].reshape(W, 16, lanes)
            for b8 in range(2):
                cols = raw[:, 8 * b8:8 * b8 + 8]
                one = jnp.transpose(cols[0:8], (1, 0, 2))
                two = jnp.transpose(cols[8:16], (1, 0, 2))
                tail = jnp.transpose(jnp.concatenate([cols[16:20], cols[16:20]], axis=0), (1, 0, 2))
                for quad in range(2):
                    b0 = 4 * quad
                    parts = []
                    for b in range(b0, b0 + 4):
                        parts += [one[b], two[b]]
                    parts += [jnp.where(lowb, tail[b0], tail[b0 + 1]), jnp.where(lowb, tail[b0 + 2], tail[b0 + 3])]
                    at = pl.ds(pl.multiple_of(g * block + 160 * b8 + 80 * quad, 16), 80)
                    for k, v in enumerate(split3(jnp.concatenate(parts, axis=0))):
                        rts[k, at, e * lanes:(e + 1) * lanes] = v

    for off in range(1, 4):
        r_quarter(off, me_r).wait_send()
        pass_on(off, me_l, across, rx_s, rx_r).wait_send()
        pass_on(off, me_l, mate, rm_s, rm_r).wait_send()
        pass_on(off, across, mate, rn_s, rn_r).wait_send()

    def norm_start():
        part = zero
        for h in range(2):
            for s in range(S):
                w = (qg[h, s, own, :] - coef(0, (bl, lt)) * vg[h, s, own, :]) * coef(1, (bl, lt))
                part = part + fold(w * w)
        sum_start((part, zero), 1, *sums)

    def norm_end(j):
        gamma = jnp.sqrt(sum_end(1, *sums)[0] / cfg.elems)
        beta = gamma * cf[4]
        out_s[STEPS + j] = beta
        cf[2] = beta * cf[3]
        cf[3] = 1.0 / gamma
        sum_sent(1, *sums)

    @pl.loop(0, STEPS)
    def _(j):
        update(0, j)
        group(0, ub0, ub1, do_w=False)

        @pl.when(j > 0)
        def _():
            norm_end(j - 1)

        group(1, ub1, ub0)

        @pl.loop(1, groups)
        def _(p):
            @pl.when(p == groups // 2)
            def _():
                update(1, j)

            group(2 * p, ub0, ub1)
            group(2 * p + 1, ub1, ub0)

        group(2 * groups, ub0, ub1, do_r=False)
        al[...] = jnp.zeros((16, 128), F32)
        acc[...] = jnp.zeros((rows, lt), F32)

        @pl.loop(0, 8 * trips)
        def _(n):
            l_trip(n)

            @pl.when(lax.rem(n, trips) == trips - 1)
            def _():
                send_on(n // trips, j)
                acc[...] = jnp.zeros((rows, lt), F32)

        sum_start((al[0:8], al[8:16]), 0, *sums)
        dot, square = sum_end(0, *sums)
        alpha = cf[3] * (dot / cfg.elems)
        size = jnp.sqrt(square / cfg.elems)
        size = jnp.where(size > 0.0, size, 1.0)
        out_s[j] = alpha
        cf[0] = alpha * cf[3]
        cf[1] = 1.0 / size
        cf[4] = size
        norm_start()

        @pl.when(j < STEPS - 1)
        def _():
            ag_start(1)

        sum_sent(0, *sums)

    norm_end(STEPS - 1)
    get_l(0).wait()
    for h in range(2):
        for s in range(S):
            v = (qg[h, s, own, :] - coef(0, (bl, lt)) * vg[h, s, own, :]) * coef(1, (bl, lt))
            qg[h, s, own, :] = v * coef(3, (bl, lt))
    result = pltpu.make_async_copy(qg.at[:, :, own, :], out_v, qsem)
    result.start()
    result.wait()


def steps(cfg, l3, rb3, psi, wl):
    lt, bl, nb, rows = cfg.lt, cfg.bl, cfg.nb, cfg.rows
    hbm = pl.BlockSpec(memory_space=pl.ANY)
    vm = pl.BlockSpec(memory_space=pltpu.VMEM)
    dma = pltpu.SemaphoreType.DMA
    block = (cfg.nl, rows, lt // cfg.nl)
    scratch = [
        pltpu.VMEM((W, rows, cfg.a), F32),
        pltpu.VMEM((3, W * bl, nb), BF),
        pltpu.VMEM((3, S, nb, lt), BF),
        pltpu.VMEM((2, S, nb, lt), F32),
        pltpu.VMEM((2, S, nb, lt), F32),
        pltpu.VMEM((2, CH, cfg.a, lt), F32),
        pltpu.VMEM((3, *block), F32),
        pltpu.VMEM(block, F32),
        pltpu.VMEM(block, F32),
        pltpu.VMEM((2, *block), F32),
        pltpu.VMEM((4, 4 * W, lt), F32),
        pltpu.VMEM((2, S, bl, lt), F32),
        pltpu.VMEM((rows, lt), F32),
        pltpu.VMEM((5, 8, 128), F32),
        pltpu.VMEM((16, 128), F32),
        pltpu.VMEM((3, 16, 128), F32),
        pltpu.VMEM((3, 16, 16, 128), F32),
        dma((2,)), dma((4,)), dma, dma((3, 16)), dma((3, 16)), dma((3,)), dma((4,)), dma((2, 4)), dma((2, 4)),
        dma((4,)), dma((4,)), dma((4,)), dma((4,)), dma((4,)), dma((4,)), dma((4,)), dma((4,)),
        pltpu.SemaphoreType.REGULAR((2,)),
    ]
    return pl.pallas_call(
        functools.partial(kernel, cfg),
        out_shape=(
            jax.ShapeDtypeStruct((2, S, bl, lt), F32),
            jax.ShapeDtypeStruct((2 * STEPS, 8, 128), F32),
        ),
        in_specs=[hbm, hbm, hbm, vm],
        out_specs=(hbm, vm),
        scratch_shapes=scratch,
        compiler_params=pltpu.CompilerParams(collective_id=0, has_side_effects=True, vmem_limit_bytes=VM_LIMIT),
    )(l3, rb3, psi, wl)


def mpo_rows(mpo_two):
    w = mpo_two.reshape(W, W, S, S).transpose(0, 3, 2, 1)
    w = jnp.concatenate([w[..., :16].reshape(W * S, 64), w[..., 16:].reshape(W * S, 16)], axis=1)
    one = lax.reduce_precision(w, 8, 7)
    two = lax.reduce_precision(w - one, 8, 7)
    three = w - one - two
    none = jnp.zeros_like(w)
    left = jnp.concatenate([
        jnp.concatenate([one, one, one], 1),
        jnp.concatenate([two, two, none], 1),
        jnp.concatenate([three, none, none], 1)], 0)
    return jnp.pad(left, ((0, 0), (0, 16))).astype(BF)


def build(mesh, cfg):
    def lanczos(psi_block, left_env, right_env, mpo_two):
        lt, a, bl = cfg.lt, cfg.a, cfg.bl
        l3 = jnp.transpose(left_env, (1, 0, 2))
        rb3 = jnp.transpose(right_env, (1, 0, 2))
        psi = psi_block.reshape(4, a, bl)
        wl = mpo_rows(mpo_two)
        vec, scal = steps(cfg, l3, rb3, psi, wl)
        vec = vec.transpose(0, 3, 1, 2).reshape(psi_block.shape)
        return scal[:STEPS, 0, 0], scal[STEPS:, 0, 0], vec

    return jax.shard_map(
        lanczos,
        mesh=mesh,
        in_specs=(P('left', None, None, 'right'), P('left', None, None), P('right', None, None), P()),
        out_specs=(P(), P(), P('left', None, None, 'right')),
        check_vma=False,
    )


def solution(mesh):
    return build(mesh, Cfg())
```
